32 devices in a mesh: row: 8 (over y, x, core), col: 4 (over z).
Axes of the slice: x: 2, y: 2, z: 4, core: 2. Of those that a mesh axis runs over, the one named last changes fastest.
Arguments:
- samples: float32 [32768, 32], P(('row', 'col')), may hold values from -3 to 3
- sample_logw: float32 [32768], P(('row', 'col')), may hold values from -8 to 8
- references: float32 [65536, 32], P(('row', 'col')), may hold values from -3 to 3
- reference_logw: float32 [65536], P(('row', 'col')), may hold values from -8 to 8
- dual_start: float32 [8, 4096], P('row'), may hold values from -3 to 3
- kept_tiles: int32 [8, 4, 32], P('row', 'col'), may hold values from 0 to 255, as said below
- tile_counts: int32 [8, 4], P('row', 'col'), may hold values from 4 to 32, as said below
Outputs:
- row_duals: float32 [8, 4096], P('row')
- col_duals: float32 [4, 16384], P('col')
The draws below stay inside these ranges and needn't reach their ends.
Inputs may be any that keep to these rules, and one draw needn't show every extreme that they name: `kept_tiles`: on device (i, j) the first tile_counts[i, j] entries are distinct tiles r * 32 + c of its 8 by 32 grid; later entries are tiles of that grid and unused. Every block of every sample group and of every reference group lies in some used tile. `tile_counts`: 32 on at least one device.
All inputs are finite; a program needn't handle non-finite values.
Results may differ from the reference program's by a relative error of at most 0.0003.
Values sent between devices are 32-bit elements; how exact they have to be, the bound alone decides.
No kernel may reach another device: no remote copies, remote signals or barrier semaphores. Data moves between devices by JAX's collectives and lax.ppermute only.
A program may use at most 64 MiB of HBM per device.

```python
import jax
import jax.numpy as jnp
from jax import lax

TILE = 512
DIM = 32
ITERS = 3
KSLOT = 32
RBD = 8
CBD = 32
SAMPLES = 32768
POINTS = 65536
N_ROW = 8
N_COL = 4


def guaranteed():
    return max((RBD + N_COL - 1) // N_COL, (CBD + N_ROW - 1) // N_ROW)


def draw_kept_tiles(key, part):
    count_guard = guaranteed()
    cells = RBD * CBD

    def single(index):
        row_index = index // N_COL
        col_index = index % N_COL
        places = jnp.arange(count_guard, dtype=jnp.int32)
        rows = (col_index + N_COL * places) % RBD
        cols = (row_index + N_ROW * places) % CBD
        chosen = rows * CBD + cols
        scores = jax.random.permutation(jax.random.fold_in(jax.random.fold_in(key, 7), index), cells).astype(jnp.int32) + count_guard
        scores = scores.at[chosen].set(places)
        order = jnp.argsort(scores, stable=True)
        return order[:KSLOT].astype(jnp.int32)
    tiles = jax.vmap(single)(jnp.arange(N_ROW * N_COL, dtype=jnp.int32))
    return tiles.reshape(N_ROW, N_COL, KSLOT)


def draw_tile_counts(key, part):
    bottom = guaranteed()
    pairs = N_ROW // 2 * N_COL
    heavy = jax.random.randint(jax.random.fold_in(key, 11), (pairs,), bottom, KSLOT + 1, dtype=jnp.int32)
    busiest = jax.random.randint(jax.random.fold_in(key, 13), (), 0, pairs, dtype=jnp.int32)
    heavy = heavy.at[busiest].set(KSLOT)
    light_top = KSLOT + bottom - heavy + 1
    light = jax.random.randint(jax.random.fold_in(key, 19), (pairs,), bottom, light_top, dtype=jnp.int32)
    light = light.at[busiest].set(bottom)
    flips = jax.random.randint(jax.random.fold_in(key, 23), (pairs,), 0, 2, dtype=jnp.int32)
    first = jnp.where(flips == 0, heavy, light)
    second = jnp.where(flips == 0, light, heavy)
    first = first.reshape(N_ROW // 2, N_COL)
    second = second.reshape(N_ROW // 2, N_COL)
    counts = jnp.stack([first, second], axis=1).reshape(N_ROW, N_COL)
    return counts.astype(jnp.int32)


def draw_dual_start(key, part):
    values = jnp.clip(jax.random.normal(jax.random.fold_in(key, 17), (N_ROW, RBD * TILE), jnp.float32), -3.0, 3.0)
    return values


def block_levels(key, shape, shards, least, top_value):
    gain = 1.0
    for dim, parts in shards:
        heights = jax.random.uniform(jax.random.fold_in(jax.random.fold_in(key, 6), dim), (parts,), jnp.float32, least / len(shards), top_value / len(shards))
        gain = gain * jnp.repeat(jnp.exp(heights), shape[dim] // parts).reshape((-1,) + (1,) * (len(shape) - 1 - dim))
    return gain


def centred(stream_key, extent, spread, limit, cuts=(), held_as=jnp.bfloat16):
    values = spread * jax.random.normal(stream_key, extent, jnp.float32)
    if cuts:
        values = values * block_levels(stream_key, extent, cuts, -0.22, 0.18)
    return jnp.clip(values, -limit, limit).astype(held_as)


def setup_inputs(seed: int = 0) -> dict:
    splits = jax.random.split(jax.random.key(seed), 8)
    return {
        "samples": centred(splits[0], (SAMPLES, DIM), 0.5, 3.0, ((0, 32),), jnp.float32),
        "sample_logw": centred(splits[1], (SAMPLES,), 2.0, 8.0, ((0, 32),), jnp.float32),
        "references": centred(splits[2], (POINTS, DIM), 0.5, 3.0, ((0, 32),), jnp.float32),
        "reference_logw": centred(splits[3], (POINTS,), 2.0, 8.0, ((0, 32),), jnp.float32),
        "dual_start": draw_dual_start(jax.random.fold_in(splits[7], 71), 0),
        "kept_tiles": draw_kept_tiles(jax.random.fold_in(splits[7], 71), 0),
        "tile_counts": draw_tile_counts(jax.random.fold_in(splits[7], 71), 0),
    }


lowest = -1.0e30
epsilon = 0.1


def combine(left, right):
    peak = jnp.maximum(left[0], right[0])
    return (peak, left[1] * jnp.exp(left[0] - peak) + right[1] * jnp.exp(right[0] - peak))


def tile_cost(row_points, col_points):
    inner = jnp.dot(row_points, col_points.T, precision=lax.Precision.HIGHEST, preferred_element_type=jnp.float32)
    row_norms = jnp.sum(row_points * row_points, axis=1)
    col_norms = jnp.sum(col_points * col_points, axis=1)
    return row_norms[:, None] + col_norms[None, :] - 2.0 * inner


def partials(x_group, x_weights, y_group, y_weights, duals, tiles, count, by_column):
    width = y_group.shape[0] if by_column else x_group.shape[0]
    col_blocks = y_group.shape[0] // TILE

    def visit(carry, slot):
        tile = tiles[slot]
        row_start = ((tile // col_blocks) * TILE).astype(jnp.int32)
        col_start = ((tile % col_blocks) * TILE).astype(jnp.int32)
        row_points = lax.dynamic_slice_in_dim(x_group, row_start, TILE, 0)
        col_points = lax.dynamic_slice_in_dim(y_group, col_start, TILE, 0)
        cost = tile_cost(row_points, col_points)
        if by_column:
            weights = lax.dynamic_slice_in_dim(x_weights, row_start, TILE, 0)
            dual_part = lax.dynamic_slice_in_dim(duals, row_start, TILE, 0)
            score = weights[:, None] + (dual_part[:, None] - cost) / epsilon
            peak = jnp.max(score, axis=0)
            total = jnp.sum(jnp.exp(score - peak[None, :]), axis=0)
            start = col_start
        else:
            weights = lax.dynamic_slice_in_dim(y_weights, col_start, TILE, 0)
            dual_part = lax.dynamic_slice_in_dim(duals, col_start, TILE, 0)
            score = weights[None, :] + (dual_part[None, :] - cost) / epsilon
            peak = jnp.max(score, axis=1)
            total = jnp.sum(jnp.exp(score - peak[:, None]), axis=1)
            start = row_start
        valid = slot < count
        peak = jnp.where(valid, peak, lowest)
        total = jnp.where(valid, total, 0.0)
        before = (lax.dynamic_slice_in_dim(carry[0], start, TILE, 0), lax.dynamic_slice_in_dim(carry[1], start, TILE, 0))
        merged = combine(before, (peak, total))
        return (lax.dynamic_update_slice_in_dim(carry[0], merged[0], start, 0), lax.dynamic_update_slice_in_dim(carry[1], merged[1], start, 0)), None

    start_state = (jnp.full((width,), lowest, jnp.float32), jnp.zeros((width,), jnp.float32))
    result, unused = lax.scan(visit, start_state, jnp.arange(tiles.shape[0], dtype=jnp.int32))
    return result


def reference(samples, sample_logw, references, reference_logw, dual_start, kept_tiles, tile_counts):
    row_width = RBD * TILE
    col_width = CBD * TILE
    x_groups = samples.reshape(N_ROW, row_width, DIM)
    x_weights = sample_logw.reshape(N_ROW, row_width)
    y_groups = references.reshape(N_ROW, N_COL, col_width // N_ROW, DIM).transpose(1, 0, 2, 3).reshape(N_COL, col_width, DIM)
    y_weights = reference_logw.reshape(N_ROW, N_COL, col_width // N_ROW).transpose(1, 0, 2).reshape(N_COL, col_width)
    devices = jnp.arange(N_ROW * N_COL, dtype=jnp.int32)

    def column_pass(row_duals):
        def single(index):
            row_index = index // N_COL
            col_index = index % N_COL
            return partials(x_groups[row_index], x_weights[row_index], y_groups[col_index], y_weights[col_index], row_duals[row_index], kept_tiles[row_index, col_index], tile_counts[row_index, col_index], True)

        peaks, totals = lax.map(single, devices)
        peaks = peaks.reshape(N_ROW, N_COL, col_width)
        totals = totals.reshape(N_ROW, N_COL, col_width)
        peak = jnp.max(peaks, axis=0)
        total = jnp.sum(totals * jnp.exp(peaks - peak[None]), axis=0)
        return -epsilon * (peak + jnp.log(total))

    def row_pass(col_duals):
        def single(index):
            row_index = index // N_COL
            col_index = index % N_COL
            return partials(x_groups[row_index], x_weights[row_index], y_groups[col_index], y_weights[col_index], col_duals[col_index], kept_tiles[row_index, col_index], tile_counts[row_index, col_index], False)

        peaks, totals = lax.map(single, devices)
        peaks = peaks.reshape(N_ROW, N_COL, row_width)
        totals = totals.reshape(N_ROW, N_COL, row_width)
        peak = jnp.max(peaks, axis=1)
        total = jnp.sum(totals * jnp.exp(peaks - peak[:, None]), axis=1)
        return -epsilon * (peak + jnp.log(total))

    row_duals = dual_start
    col_duals = jnp.zeros((N_COL, col_width), jnp.float32)
    for turn in range(ITERS):
        col_duals = column_pass(row_duals)
        row_duals = row_pass(col_duals)
    return row_duals, col_duals
```

```python
import functools
import math

import jax
import jax.numpy as jnp
from jax import lax
from jax.experimental import pallas as pl
from jax.experimental.pallas import tpu as pltpu
from jax.sharding import PartitionSpec as P

TILE = 512
ITERS = 3
LANES = 128
BIAS = 16

lowest = -1e30
epsilon = 0.1
log2e = math.log2(math.e)
ln2 = math.log(2.0)

VM = pl.BlockSpec(memory_space=pltpu.VMEM)
SM = pl.BlockSpec(memory_space=pltpu.SMEM)
PARAMS = pltpu.CompilerParams(vmem_limit_bytes=24 * 1024 * 1024)


def swap(value, axis, distance):
    pairs = [(i, i ^ distance) for i in range(lax.axis_size(axis))]
    return jax.tree.map(lambda part: lax.ppermute(part, axis, pairs), value)


def pack_kernel(xt_ref, wx_ref, yt_ref, wy_ref, x_ref, keep_ref, *send_refs):
    dim = xt_ref.shape[0]
    chunks = TILE // LANES

    def put(out, b, points_ref, weights_ref, block):
        for j in range(chunks):
            start = pl.multiple_of(block * TILE + j * LANES, LANES)
            out[b, j * dim : (j + 1) * dim, :] = points_ref[:, pl.ds(start, LANES)]
        out[b, chunks * dim : chunks * dim + chunks, :] = weights_ref[pl.ds(block * chunks, chunks), :]

    for b in range(x_ref.shape[0]):
        put(x_ref, b, xt_ref, wx_ref, b)
    if send_refs:
        parity = lax.rem(lax.axis_index("row"), 2)
        for b in range(keep_ref.shape[0]):
            put(keep_ref, b, yt_ref, wy_ref, 2 * b + parity)
            put(send_refs[0], b, yt_ref, wy_ref, 2 * b + 1 - parity)
    else:
        for b in range(keep_ref.shape[0]):
            put(keep_ref, b, yt_ref, wy_ref, b)


def prepare(own_x, partner_x, own_y, partner_y, dual_own, dual_partner, tiles_own, tiles_partner, sizes):
    row_blocks, col_blocks, dim = sizes
    n_x, n_y = len(own_x), len(own_y)
    both = len(partner_y) > 0
    slots = tiles_own.shape[0] - 1
    per_x = own_x[0].shape[0]
    per_y = own_y[0].shape[0] * (2 if both else 1)
    half_cols = col_blocks // 2
    all_rows = 2 * row_blocks
    chunks = TILE // LANES

    def kernel(*refs):
        refs = list(refs)

        def take(n):
            out = refs[:n]
            del refs[:n]
            return out

        xs, pxs, ys, pys = take(n_x), take(n_x), take(n_y), take(len(partner_y))
        d_own, d_partner, t_own, t_partner = take(4)
        xp, yp, u0, wx, wy, nx, ny, m_list, n_list, count = take(10)
        row, col = lax.axis_index("row"), lax.axis_index("col")
        parity = lax.rem(row, 2)
        pair = lax.div(row, 2)

        def load(ref, b):
            points = jnp.concatenate([ref[b, j * dim : (j + 1) * dim, :] for j in range(chunks)], axis=1)
            base = chunks * dim
            weights = jnp.concatenate([ref[b, base + j : base + j + 1, :] for j in range(chunks)], axis=1)
            return points, weights

        def split(out, index, points):
            high = points.astype(jnp.bfloat16)
            low = (points - high.astype(jnp.float32)).astype(jnp.bfloat16)
            out[index, 0:dim, :] = high
            out[index, dim : 2 * dim, :] = low

        for group, (sources, duals) in enumerate(((xs, d_own), (pxs, d_partner))):
            side = parity if group == 0 else 1 - parity
            for d in range(n_x):
                for b in range(per_x):
                    local = (col ^ d) * per_x + b
                    index = side * row_blocks + local
                    points, weights = load(sources[d], b)
                    norm = jnp.sum(points * points, axis=0, keepdims=True)
                    split(xp, index, points * (2.0 * log2e / epsilon))
                    start = pl.multiple_of(local * TILE, TILE)
                    dual = duals[0:1, pl.ds(start, TILE)]
                    u0[pl.ds(index, 1), :] = log2e * weights + (dual - norm) * (log2e / epsilon)
                    wx[pl.ds(index, 1), :] = log2e * weights
                    nx[pl.ds(index, 1), :] = norm
        for d in range(n_y):
            place = pair ^ d
            for from_partner in range(2 if both else 1):
                source = (ys, pys)[from_partner][d]
                here = source.shape[0]
                for b in range(here):
                    index = place * per_y + b
                    if both:
                        index = index + (parity if from_partner == 0 else 1 - parity) * here
                    points, weights = load(source, b)
                    norm = jnp.sum(points * points, axis=0, keepdims=True)
                    split(yp, index, points)
                    wy[pl.ds(index, 1), :] = log2e * weights
                    ny[pl.ds(index, 1), :] = norm

        def collect(ref, side, filled):
            def visit(k, filled):
                tile = ref[k]
                r, c = lax.div(tile, col_blocks), lax.rem(tile, col_blocks)

                @pl.when(lax.rem(c, 2) == parity)
                def _():
                    m_list[filled] = side * row_blocks + r
                    n_list[filled] = lax.div(c, 2)

                return filled + (lax.rem(c, 2) == parity).astype(jnp.int32)

            return lax.fori_loop(0, ref[slots], visit, filled)

        filled = collect(t_own, parity, jnp.int32(0))
        filled = collect(t_partner, 1 - parity, filled)
        count[0] = filled
        m_list[filled] = 0
        n_list[filled] = 0
        m_list[filled + 1] = 0
        n_list[filled + 1] = 0

    f32, bf16, i32 = jnp.float32, jnp.bfloat16, jnp.int32
    shape = jax.ShapeDtypeStruct
    rows, cols = (all_rows, TILE), (half_cols, TILE)
    capacity = 2 * slots + 2
    return pl.pallas_call(
        kernel,
        out_shape=(
            shape((all_rows, 2 * dim, TILE), bf16),
            shape((half_cols, 2 * dim, TILE), bf16),
            shape(rows, f32),
            shape(rows, f32),
            shape(cols, f32),
            shape(rows, f32),
            shape(cols, f32),
            shape((capacity,), i32),
            shape((capacity,), i32),
            shape((1,), i32),
        ),
        in_specs=[VM] * (2 * n_x + n_y + len(partner_y) + 2) + [SM] * 2,
        out_specs=(VM,) * 7 + (SM,) * 3,
        compiler_params=PARAMS,
        name="prepare",
    )(*own_x, *partner_x, *own_y, *partner_y, dual_own, dual_partner, tiles_own, tiles_partner)


def log_sum(parts):
    if len(parts) == 1:
        return parts[0]
    peak = functools.reduce(jnp.maximum, parts)
    total = functools.reduce(jnp.add, [jnp.exp2(part - peak) for part in parts])
    return peak + jnp.log2(total)


def half_step(from_points, to_points, weights, parts, m_list, n_list, count, from_first, keep_total):
    m_blocks, width, _ = from_points.shape
    n_blocks = to_points.shape[0]
    dim = width // 2
    n_parts = len(parts)
    groups = TILE // 8

    def kernel(*refs):
        m_idx, n_idx, size, a_ref, b_ref = refs[:5]
        if n_parts:
            w_ref, part_refs = refs[5], refs[6 : 6 + n_parts]
            out_refs = refs[6 + n_parts :]
        else:
            w_ref, part_refs, out_refs = refs[5], (), refs[6:]
        out_ref = out_refs[0]
        scratch = out_refs[2:] if keep_total else out_refs[1:]
        bias, peaks, sums, s0, s1, p0, p1 = scratch

        if n_parts:
            total = log_sum([ref[...] for ref in part_refs])
            if keep_total:
                out_refs[1][...] = total
            lift = w_ref[...] - total
        else:
            lift = w_ref[...]
        high = lift.astype(jnp.bfloat16).astype(jnp.float32)
        rest = lift - high
        middle = rest.astype(jnp.bfloat16).astype(jnp.float32)
        low = rest - middle
        place = lax.broadcasted_iota(jnp.int32, (BIAS, TILE), 0)
        for i in range(m_blocks):
            rows = jnp.where(
                place == 0,
                high[i : i + 1, :],
                jnp.where(place == 1, middle[i : i + 1, :], jnp.where(place == 2, low[i : i + 1, :], 0.0)),
            )
            bias[i] = rows.astype(jnp.bfloat16)
        peaks[...] = jnp.full(peaks.shape, lowest, jnp.float32)
        sums[...] = jnp.zeros(sums.shape, jnp.float32)
        ones = jnp.where(place < 3, 1.0, 0.0).astype(jnp.bfloat16)
        n = size[0]

        def doubled(ref, i, high_first):
            both = ref[i]
            if high_first:
                return [both[0:dim], both]
            return [both, both[0:dim]]

        def scores(k, score, peak):
            k = jnp.minimum(k, n)
            m, c = m_idx[k], n_idx[k]
            left = jnp.concatenate(doubled(a_ref, m, not from_first) + [bias[m]], axis=0)
            right = jnp.concatenate(doubled(b_ref, c, from_first) + [ones], axis=0)
            value = lax.dot_general(left, right, (((0,), (0,)), ((), ())), preferred_element_type=jnp.float32)
            value = value.reshape(groups, 8, TILE)
            score[...] = value
            peak[...] = jnp.max(value, axis=0)

        def absorb(k, score, peak):
            c = jnp.where(k < n, n_idx[jnp.minimum(k, n)], n_blocks)
            before = peaks[c]
            after = jnp.maximum(before, peak[...])
            total = jnp.sum(jnp.exp2(score[...] - after[None]), axis=0)
            sums[c] = sums[c] * jnp.exp2(before - after) + total
            peaks[c] = after

        scores(0, s0, p0)

        def visit(step, carry):
            scores(2 * step + 1, s1, p1)
            absorb(2 * step, s0, p0)
            scores(2 * step + 2, s0, p0)
            absorb(2 * step + 1, s1, p1)
            return carry

        lax.fori_loop(0, lax.div(n + 1, 2), visit, 0)
        top = peaks[0:n_blocks]
        peak = jnp.max(top, axis=1)
        total = jnp.sum(sums[0:n_blocks] * jnp.exp2(top - peak[:, None, :]), axis=1)
        out_ref[...] = jnp.where(total > 0.0, peak + jnp.log2(total), lowest)

    f32 = jnp.float32
    shape = jax.ShapeDtypeStruct
    out_shape = [shape((n_blocks, TILE), f32)] + ([shape((m_blocks, TILE), f32)] if keep_total else [])
    return pl.pallas_call(
        kernel,
        out_shape=out_shape,
        in_specs=[SM] * 3 + [VM] * (3 + n_parts),
        out_specs=[VM] * len(out_shape),
        scratch_shapes=[
            pltpu.VMEM((m_blocks, BIAS, TILE), jnp.bfloat16),
            pltpu.VMEM((n_blocks + 1, 8, TILE), f32),
            pltpu.VMEM((n_blocks + 1, 8, TILE), f32),
            pltpu.VMEM((groups, 8, TILE), f32),
            pltpu.VMEM((groups, 8, TILE), f32),
            pltpu.VMEM((8, TILE), f32),
            pltpu.VMEM((8, TILE), f32),
        ],
        compiler_params=PARAMS,
        name="column_step" if from_first else "row_step",
    )(m_list, n_list, count, from_points, to_points, weights, *parts)


def per_device(samples, sample_logw, references, reference_logw, dual_start, kept_tiles, tile_counts):
    n_row, n_col = lax.axis_size("row"), lax.axis_size("col")
    dim = samples.shape[1]
    own_row_blocks = samples.shape[0] // TILE
    own_col_blocks = references.shape[0] // TILE
    row_blocks, col_blocks = own_row_blocks * n_col, own_col_blocks * n_row
    chunks = TILE // LANES
    parity = lax.axis_index("row") % 2
    both = own_col_blocks % 2 == 0
    assert both or own_col_blocks == 1

    shape = jax.ShapeDtypeStruct
    depth = chunks * (dim + 1)
    kept = own_col_blocks // 2 if both else own_col_blocks
    packed_shapes = [shape((own_row_blocks, depth, LANES), jnp.float32)]
    packed_shapes += [shape((kept, depth, LANES), jnp.float32)] * (2 if both else 1)
    packed = pl.pallas_call(
        pack_kernel,
        out_shape=packed_shapes,
        in_specs=[VM] * 4,
        out_specs=[VM] * len(packed_shapes),
        compiler_params=PARAMS,
        name="pack",
    )(
        samples.T,
        sample_logw.reshape(-1, LANES),
        references.T,
        reference_logw.reshape(-1, LANES),
    )
    x_pack, y_keep = packed[0], packed[1]
    own_y = [y_keep] + [swap(y_keep, "row", 2 * d) for d in range(1, n_row // 2)]
    partner_y = []
    if both:
        y_other = swap(packed[2], "row", 1)
        partner_y = [y_other] + [swap(y_other, "row", 2 * d) for d in range(1, n_row // 2)]
    own_x = [x_pack] + [swap(x_pack, "col", d) for d in range(1, n_col)]
    partner_x = [swap(part, "row", 1) for part in own_x]
    dual_partner = swap(dual_start, "row", 1)
    tiles_own = jnp.concatenate([kept_tiles[0, 0], tile_counts[0]])
    tiles_partner = swap(tiles_own, "row", 1)
    xp, yp, start, wx, wy, nx, ny, m_list, n_list, count = prepare(
        own_x, partner_x, own_y, partner_y, dual_start, dual_partner,
        tiles_own, tiles_partner, (row_blocks, col_blocks, dim),
    )

    row_parts = []
    for turn in range(ITERS):
        last = turn == ITERS - 1
        (part,) = half_step(xp, yp, wx if turn else start, row_parts, m_list, n_list, count, True, False)
        col_parts = [part] + [swap(part, "row", 2 * d) for d in range(1, n_row // 2)]
        part, *kept_total = half_step(yp, xp, wy, col_parts, n_list, m_list, count, False, last)
        part = log_sum([part, swap(part, "row", 1)])
        row_parts = [part] + [swap(part, "col", d) for d in range(1, n_col)]

    own = [lax.dynamic_slice_in_dim(part, parity * row_blocks, row_blocks, 0) for part in row_parts]
    norms = lax.dynamic_slice_in_dim(nx, parity * row_blocks, row_blocks, 0)
    row_duals = norms - (epsilon * ln2) * log_sum(own)
    col_half = ny - (epsilon * ln2) * kept_total[0]
    col_other = swap(col_half, "row", 1)
    even = jnp.where(parity == 0, col_half, col_other)
    odd = jnp.where(parity == 0, col_other, col_half)
    col_duals = jnp.stack([even, odd], axis=1)
    return (row_duals.reshape(1, -1), col_duals.reshape(1, -1))


def solution(mesh):
    return jax.shard_map(
        per_device,
        mesh=mesh,
        in_specs=(
            P(("row", "col"), None),
            P(("row", "col")),
            P(("row", "col"), None),
            P(("row", "col")),
            P("row", None),
            P("row", "col", None),
            P("row", "col"),
        ),
        out_specs=(P("row", None), P("col", None)),
        check_vma=False,
    )
```

```python
import functools
import math

import jax
import jax.numpy as jnp
from jax import lax
from jax.experimental import pallas as pl
from jax.experimental.pallas import tpu as pltpu
from jax.sharding import PartitionSpec as P

TILE = 512
ITERS = 3
LANES = 128
BIAS = 16
SHIFT = 12
CODE = 1 << SHIFT
UNROLL = 4
SAMPLE = 128
MARGIN = 80.0

lowest = -1e30
epsilon = 0.1
log2e = math.log2(math.e)
ln2 = math.log(2.0)


VM = pl.BlockSpec(memory_space=pltpu.VMEM)
HBM = pl.BlockSpec(memory_space=pltpu.HBM)
SM = pl.BlockSpec(memory_space=pltpu.SMEM)
PARAMS = pltpu.CompilerParams(vmem_limit_bytes=24 * 1024 * 1024)


def swap(value, axis, distance):
    pairs = [(i, i ^ distance) for i in range(lax.axis_size(axis))]
    return jax.tree.map(lambda part: lax.ppermute(part, axis, pairs), value)


def pack_kernel(xt_ref, wx_hbm, yt_ref, wy_hbm, *refs):
    *outs, wx_ref, wy_ref, sem = refs
    dim = xt_ref.shape[0]
    chunks = TILE // LANES
    copies = [(wx_hbm, wx_ref), (wy_hbm, wy_ref)]
    stores = []

    def put(out, b, points_ref, weights_ref, block):
        start = pl.multiple_of(block * TILE, TILE)
        for j in range(chunks):
            source = points_ref.at[:, pl.ds(start + j * LANES, LANES)]
            copies.append((source, out.at[b, pl.ds(j * dim, dim), :]))
        stores.append((out, b, weights_ref, block))

    x_ref, keep_ref, *send_refs = outs
    for b in range(x_ref.shape[0]):
        put(x_ref, b, xt_ref, wx_ref, b)
    if send_refs:
        parity = lax.rem(lax.axis_index("row"), 2)
        for b in range(keep_ref.shape[0]):
            put(send_refs[0], b, yt_ref, wy_ref, 2 * b + 1 - parity)
        for b in range(keep_ref.shape[0]):
            put(keep_ref, b, yt_ref, wy_ref, 2 * b + parity)
    else:
        for b in range(keep_ref.shape[0]):
            put(keep_ref, b, yt_ref, wy_ref, b)
    started = [pltpu.make_async_copy(a, b, sem.at[i]) for i, (a, b) in enumerate(copies)]
    for copy in started:
        copy.start()
    for copy in started[:2]:
        copy.wait()
    for out, b, weights_ref, block in stores:
        out[b, chunks * dim : chunks * (dim + 1), :] = weights_ref[pl.ds(block * chunks, chunks), :]
    for copy in started[2:]:
        copy.wait()


def collect_tiles(tiles_own, tiles_partner, row_blocks, col_blocks):
    slots = tiles_own.shape[0] - 1

    def kernel(t_own, t_partner, found):
        parity = lax.rem(lax.axis_index("row"), 2)

        def collect(ref, side, filled):
            def visit(k, filled):
                tile = ref[k]
                r, c = lax.div(tile, col_blocks), lax.rem(tile, col_blocks)
                found[filled] = (side * row_blocks + r) * CODE + lax.div(c, 2)
                return filled + (lax.rem(c, 2) == parity).astype(jnp.int32)

            return lax.fori_loop(0, ref[slots], visit, filled)

        filled = collect(t_own, parity, jnp.int32(1))
        filled = collect(t_partner, 1 - parity, filled)
        found[0] = filled - 1
        found[filled] = 0

    return pl.pallas_call(
        kernel,
        out_shape=jax.ShapeDtypeStruct((2 * slots + 2,), jnp.int32),
        in_specs=[SM] * 2,
        out_specs=SM,
        compiler_params=PARAMS,
        name="collect",
    )(tiles_own, tiles_partner)


def prepare(own_x, partner_x, own_y, partner_y, dual_own, dual_partner, sizes):
    row_blocks, col_blocks, dim = sizes
    n_x, n_y = len(own_x), len(own_y)
    both = len(partner_y) > 0
    per_x = own_x[0].shape[0]
    per_y = own_y[0].shape[0] * (2 if both else 1)
    half_cols = col_blocks // 2
    all_rows = 2 * row_blocks
    chunks = TILE // LANES

    def kernel(*refs):
        refs = list(refs)

        def take(n):
            out = refs[:n]
            del refs[:n]
            return out

        xs, pxs, ys, pys = take(n_x), take(n_x), take(n_y), take(len(partner_y))
        d_own, d_partner = take(2)
        xp, yp, u0, wx, wy, nx, ny = take(7)
        row, col = lax.axis_index("row"), lax.axis_index("col")
        parity = lax.rem(row, 2)
        pair = lax.div(row, 2)

        def load(ref, b):
            points = jnp.concatenate([ref[b, j * dim : (j + 1) * dim, :] for j in range(chunks)], axis=1)
            base = chunks * dim
            weights = jnp.concatenate([ref[b, base + j : base + j + 1, :] for j in range(chunks)], axis=1)
            return points, weights

        def split(out, index, points):
            high = points.astype(jnp.bfloat16)
            low = (points - high.astype(jnp.float32)).astype(jnp.bfloat16)
            out[index, 0:dim, :] = high
            out[index, dim : 2 * dim, :] = low

        for group, (sources, duals) in enumerate(((xs, d_own), (pxs, d_partner))):
            side = parity if group == 0 else 1 - parity
            for d in range(n_x):
                for b in range(per_x):
                    local = (col ^ d) * per_x + b
                    index = side * row_blocks + local
                    points, weights = load(sources[d], b)
                    norm = jnp.sum(points * points, axis=0, keepdims=True)
                    split(xp, index, points * (2.0 * log2e / epsilon))
                    start = pl.multiple_of(local * TILE, TILE)
                    dual = duals[0:1, pl.ds(start, TILE)]
                    u0[pl.ds(index, 1), :] = log2e * weights + (dual - norm) * (log2e / epsilon)
                    wx[pl.ds(index, 1), :] = log2e * weights
                    nx[pl.ds(index, 1), :] = norm
        for d in range(n_y):
            place = pair ^ d
            for from_partner in range(2 if both else 1):
                source = (ys, pys)[from_partner][d]
                here = source.shape[0]
                for b in range(here):
                    index = place * per_y + b
                    if both:
                        index = index + (parity if from_partner == 0 else 1 - parity) * here
                    points, weights = load(source, b)
                    norm = jnp.sum(points * points, axis=0, keepdims=True)
                    split(yp, index, points)
                    wy[pl.ds(index, 1), :] = log2e * weights
                    ny[pl.ds(index, 1), :] = norm

    f32, bf16 = jnp.float32, jnp.bfloat16
    shape = jax.ShapeDtypeStruct
    rows, cols = (all_rows, TILE), (half_cols, TILE)
    return pl.pallas_call(
        kernel,
        out_shape=(
            shape((all_rows, 2 * dim, TILE), bf16),
            shape((half_cols, 2 * dim, TILE), bf16),
            shape(rows, f32),
            shape(rows, f32),
            shape(cols, f32),
            shape(rows, f32),
            shape(cols, f32),
        ),
        in_specs=[VM] * (2 * n_x + n_y + len(partner_y) + 2),
        out_specs=(VM,) * 7,
        compiler_params=PARAMS,
        name="prepare",
    )(*own_x, *partner_x, *own_y, *partner_y, dual_own, dual_partner)


def log_sum(parts):
    if len(parts) == 1:
        return parts[0]
    peak = functools.reduce(jnp.maximum, parts)
    total = functools.reduce(jnp.add, [jnp.exp2(part - peak) for part in parts])
    return peak + jnp.log2(total)


def half_step(from_points, to_points, weights, parts, guess, tiles, from_first, keep_total):
    m_blocks, width, _ = from_points.shape
    n_blocks = to_points.shape[0]
    dim = width // 2
    n_parts = len(parts)
    groups = TILE // 8
    guessed = guess is not None

    def kernel(*refs):
        tiles_ref, a_ref, b_ref, w_ref = refs[:4]
        part_refs = refs[4 : 4 + n_parts]
        rest = list(refs[4 + n_parts :])
        guess_ref = rest.pop(0) if guessed else None
        out_ref = rest.pop(0)
        total_ref = rest.pop(0) if keep_total else None
        lifts, drops, peaks, sums, s0, s1, p0, p1 = rest
        n = tiles_ref[0]

        def ends(k):
            code = tiles_ref[jnp.minimum(k, n) + 1]
            first, second = lax.shift_right_logical(code, SHIFT), code & (CODE - 1)
            return (first, second) if from_first else (second, first)


        if n_parts:
            total = log_sum([ref[...] for ref in part_refs])
            if keep_total:
                total_ref[...] = total
            lift = w_ref[...] - total
        else:
            lift = w_ref[...]
        place = lax.broadcasted_iota(jnp.int32, (BIAS, TILE), 0)

        def pieces(out, value, first, ones):
            high = value.astype(jnp.bfloat16).astype(jnp.float32)
            rest = value - high
            middle = rest.astype(jnp.bfloat16).astype(jnp.float32)
            low = rest - middle
            filler = jnp.where((place >= ones) & (place < ones + 3), 1.0, 0.0)
            for i in range(value.shape[0]):
                rows = filler
                for at, part in enumerate((high, middle, low)):
                    rows = jnp.where(place == first + at, part[i : i + 1, :], rows)
                out[i] = rows.astype(jnp.bfloat16)

        pieces(lifts, lift, 0, 3)
        plain = jnp.where(place < 3, 1.0, 0.0).astype(jnp.bfloat16)

        def doubled(ref, i, high_first):
            both = ref[i]
            if high_first:
                return [both[0:dim], both]
            return [both, both[0:dim]]

        def product(k, shifted, rows=TILE):
            m, c = ends(k)
            left = jnp.concatenate(doubled(a_ref, m, not from_first) + [lifts[m]], axis=0)[:, :rows]
            right = jnp.concatenate(doubled(b_ref, c, from_first) + [drops[c] if shifted else plain], axis=0)
            value = lax.dot_general(left, right, (((0,), (0,)), ((), ())), preferred_element_type=jnp.float32)
            return value.reshape(rows // 8, 8, TILE)

        def target(k):
            return jnp.where(k < n, ends(k)[1], n_blocks)

        def exact():
            peaks[...] = jnp.full(peaks.shape, lowest, jnp.float32)
            sums[...] = jnp.zeros(sums.shape, jnp.float32)

            def scores(k, score, peak):
                value = product(k, False)
                score[...] = value
                peak[...] = jnp.max(value, axis=0)

            def absorb(k, score, peak):
                c = target(k)
                before = peaks[c]
                after = jnp.maximum(before, peak[...])
                total = jnp.sum(jnp.exp2(score[...] - after[None]), axis=0)
                sums[c] = sums[c] * jnp.exp2(before - after) + total
                peaks[c] = after

            scores(0, s0, p0)

            def visit(step, carry):
                scores(2 * step + 1, s1, p1)
                absorb(2 * step, s0, p0)
                scores(2 * step + 2, s0, p0)
                absorb(2 * step + 1, s1, p1)
                return carry

            lax.fori_loop(0, lax.div(n + 1, 2), visit, 0)
            top = peaks[0:n_blocks]
            peak = jnp.max(top, axis=1)
            total = jnp.sum(sums[0:n_blocks] * jnp.exp2(top - peak[:, None, :]), axis=1)
            out_ref[...] = jnp.where(total > 0.0, peak + jnp.log2(total), lowest)

        batches = lax.div(n + UNROLL - 1, UNROLL)
        if guessed:
            shift = guess_ref[...]
        else:
            peaks[...] = jnp.full(peaks.shape, lowest, jnp.float32)

            def look(step, carry):
                found = []
                for u in range(UNROLL):
                    k = UNROLL * step + u
                    found.append((target(k), jnp.max(product(k, False, SAMPLE), axis=0)))
                for c, peak in found:
                    peaks[c] = jnp.maximum(peaks[c], peak)
                return carry

            lax.fori_loop(0, batches, look, 0)
            shift = jnp.max(peaks[0:n_blocks], axis=1) + MARGIN
        used = shift > 0.5 * lowest
        shift = jnp.where(used, shift, 0.0)
        pieces(drops, -shift, 3, 0)
        sums[...] = jnp.zeros(sums.shape, jnp.float32)

        def visit(step, carry):
            found = []
            for u in range(UNROLL):
                k = UNROLL * step + u
                value = product(k, True)
                found.append((target(k), jnp.sum(jnp.exp2(value), axis=0)))
            for c, total in found:
                sums[c] += total
            return carry

        lax.fori_loop(0, batches, visit, 0)
        total = jnp.sum(sums[0:n_blocks], axis=1)
        out_ref[...] = jnp.where(used, shift + jnp.log2(total), lowest)
        inside = (total > 2.0**-90) & (total < 2.0**120)
        outside = jnp.max(jnp.where(used & ~inside, 1.0, 0.0))
        pl.when(outside > 0.5)(exact)

    f32 = jnp.float32
    shape = jax.ShapeDtypeStruct
    out_shape = [shape((n_blocks, TILE), f32)] + ([shape((m_blocks, TILE), f32)] if keep_total else [])
    extra = (guess,) if guessed else ()
    return pl.pallas_call(
        kernel,
        out_shape=out_shape,
        in_specs=[SM] + [VM] * (3 + n_parts + len(extra)),
        out_specs=[VM] * len(out_shape),
        scratch_shapes=[
            pltpu.VMEM((m_blocks, BIAS, TILE), jnp.bfloat16),
            pltpu.VMEM((n_blocks, BIAS, TILE), jnp.bfloat16),
            pltpu.VMEM((n_blocks + 1, 8, TILE), f32),
            pltpu.VMEM((n_blocks + 1, 8, TILE), f32),
            pltpu.VMEM((groups, 8, TILE), f32),
            pltpu.VMEM((groups, 8, TILE), f32),
            pltpu.VMEM((8, TILE), f32),
            pltpu.VMEM((8, TILE), f32),
        ],
        compiler_params=PARAMS,
        name="column_step" if from_first else "row_step",
    )(tiles, from_points, to_points, weights, *parts, *extra)


def per_device(samples, sample_logw, references, reference_logw, dual_start, kept_tiles, tile_counts):
    n_row, n_col = lax.axis_size("row"), lax.axis_size("col")
    dim = samples.shape[1]
    own_row_blocks = samples.shape[0] // TILE
    own_col_blocks = references.shape[0] // TILE
    row_blocks, col_blocks = own_row_blocks * n_col, own_col_blocks * n_row
    chunks = TILE // LANES
    parity = lax.axis_index("row") % 2
    both = own_col_blocks % 2 == 0
    assert both or own_col_blocks == 1

    shape = jax.ShapeDtypeStruct
    depth = chunks * (dim + 1)
    kept = own_col_blocks // 2 if both else own_col_blocks
    packed_shapes = [shape((own_row_blocks, depth, LANES), jnp.float32)]
    packed_shapes += [shape((kept, depth, LANES), jnp.float32)] * (2 if both else 1)
    packed = pl.pallas_call(
        pack_kernel,
        out_shape=packed_shapes,
        in_specs=[HBM] * 4,
        out_specs=[VM] * len(packed_shapes),
        scratch_shapes=[
            pltpu.VMEM((own_row_blocks * chunks, LANES), jnp.float32),
            pltpu.VMEM((own_col_blocks * chunks, LANES), jnp.float32),
            pltpu.SemaphoreType.DMA((chunks * (own_row_blocks + own_col_blocks) + 2,)),
        ],
        compiler_params=PARAMS,
        name="pack",
    )(
        samples.T,
        sample_logw.reshape(-1, LANES),
        references.T,
        reference_logw.reshape(-1, LANES),
    )
    x_pack, y_keep = packed[0], packed[1]
    own_y = [y_keep] + [swap(y_keep, "row", 2 * d) for d in range(1, n_row // 2)]
    partner_y = []
    if both:
        partner_y = [swap(packed[2], "row", 2 * d + 1) for d in range(n_row // 2)]
    own_x = [x_pack] + [swap(x_pack, "col", d) for d in range(1, n_col)]
    partner_x = [swap(part, "row", 1) for part in own_x]
    dual_partner = swap(dual_start, "row", 1)
    tiles_own = jnp.concatenate([kept_tiles[0, 0], tile_counts[0]])
    tiles_partner = swap(tiles_own, "row", 1)
    tiles = collect_tiles(tiles_own, tiles_partner, row_blocks, col_blocks)
    xp, yp, start, wx, wy, nx, ny = prepare(
        own_x, partner_x, own_y, partner_y, dual_start, dual_partner, (row_blocks, col_blocks, dim)
    )

    row_parts = []
    col_guess = row_guess = None
    for turn in range(ITERS):
        last = turn == ITERS - 1
        (part,) = half_step(xp, yp, wx if turn else start, row_parts, col_guess, tiles, True, False)
        col_guess = part
        col_parts = [part] + [swap(part, "row", 2 * d) for d in range(1, n_row // 2)]
        part, *kept_total = half_step(yp, xp, wy, col_parts, row_guess, tiles, False, last)
        row_guess = part
        part = log_sum([part, swap(part, "row", 1)])
        row_parts = [part] + [swap(part, "col", d) for d in range(1, n_col)]

    own = [lax.dynamic_slice_in_dim(part, parity * row_blocks, row_blocks, 0) for part in row_parts]
    norms = lax.dynamic_slice_in_dim(nx, parity * row_blocks, row_blocks, 0)
    row_duals = norms - (epsilon * ln2) * log_sum(own)
    col_half = ny - (epsilon * ln2) * kept_total[0]
    col_other = swap(col_half, "row", 1)
    even = jnp.where(parity == 0, col_half, col_other)
    odd = jnp.where(parity == 0, col_other, col_half)
    col_duals = jnp.stack([even, odd], axis=1)
    return (row_duals.reshape(1, -1), col_duals.reshape(1, -1))


def solution(mesh):
    return jax.shard_map(
        per_device,
        mesh=mesh,
        in_specs=(
            P(("row", "col"), None),
            P(("row", "col")),
            P(("row", "col"), None),
            P(("row", "col")),
            P("row", None),
            P("row", "col", None),
            P("row", "col"),
        ),
        out_specs=(P("row", None), P("col", None)),
        check_vma=False,
    )
```

```python
import functools
import math

import jax
import jax.numpy as jnp
from jax import lax
from jax.experimental import pallas as pl
from jax.experimental.pallas import tpu as pltpu
from jax.sharding import PartitionSpec as P


TILE = 512
ITERS = 3
LANES = 128
BIAS = 16
SHIFT = 12
CODE = 1 << SHIFT
UNROLL = 8
SAMPLE = 128
MARGIN = 80.0

lowest = -1e30
epsilon = 0.1
log2e = math.log2(math.e)
ln2 = math.log(2.0)


VM = pl.BlockSpec(memory_space=pltpu.VMEM)
HBM = pl.BlockSpec(memory_space=pltpu.HBM)
SM = pl.BlockSpec(memory_space=pltpu.SMEM)
PARAMS = pltpu.CompilerParams(vmem_limit_bytes=24 * 1024 * 1024)


def swap(value, axis, distance):
    pairs = [(i, i ^ distance) for i in range(lax.axis_size(axis))]
    return jax.tree.map(lambda part: lax.ppermute(part, axis, pairs), value)


def pack_kernel(xt_ref, wx_hbm, yt_ref, wy_hbm, *refs):
    *outs, wx_ref, wy_ref, sem = refs
    dim = xt_ref.shape[0]
    chunks = TILE // LANES
    copies = [(wx_hbm, wx_ref), (wy_hbm, wy_ref)]
    stores = []

    def put(out, b, points_ref, weights_ref, block):
        start = pl.multiple_of(block * TILE, TILE)
        for j in range(chunks):
            source = points_ref.at[:, pl.ds(start + j * LANES, LANES)]
            copies.append((source, out.at[b, pl.ds(j * dim, dim), :]))
        stores.append((out, b, weights_ref, block))

    x_ref, keep_ref, *send_refs = outs
    for b in range(x_ref.shape[0]):
        put(x_ref, b, xt_ref, wx_ref, b)
    if send_refs:
        parity = lax.rem(lax.axis_index("row"), 2)
        for b in range(keep_ref.shape[0]):
            put(send_refs[0], b, yt_ref, wy_ref, 2 * b + 1 - parity)
        for b in range(keep_ref.shape[0]):
            put(keep_ref, b, yt_ref, wy_ref, 2 * b + parity)
    else:
        for b in range(keep_ref.shape[0]):
            put(keep_ref, b, yt_ref, wy_ref, b)
    started = [pltpu.make_async_copy(a, b, sem.at[i]) for i, (a, b) in enumerate(copies)]
    for copy in started:
        copy.start()
    for copy in started[:2]:
        copy.wait()
    for out, b, weights_ref, block in stores:
        out[b, chunks * dim : chunks * (dim + 1), :] = weights_ref[pl.ds(block * chunks, chunks), :]
    for copy in started[2:]:
        copy.wait()


def collect_tiles(tiles_own, tiles_partner, row_blocks, col_blocks):
    slots = tiles_own.shape[0] - 1

    def kernel(t_own, t_partner, found):
        parity = lax.rem(lax.axis_index("row"), 2)

        def collect(ref, side, filled):
            def visit(k, filled):
                tile = ref[k]
                r, c = lax.div(tile, col_blocks), lax.rem(tile, col_blocks)
                found[filled] = (side * row_blocks + r) * CODE + lax.div(c, 2)
                return filled + (lax.rem(c, 2) == parity).astype(jnp.int32)

            return lax.fori_loop(0, ref[slots], visit, filled)

        filled = collect(t_own, parity, jnp.int32(1))
        filled = collect(t_partner, 1 - parity, filled)
        found[0] = filled - 1
        found[filled] = 0

    return pl.pallas_call(
        kernel,
        out_shape=jax.ShapeDtypeStruct((2 * slots + 2,), jnp.int32),
        in_specs=[SM] * 2,
        out_specs=SM,
        compiler_params=PARAMS,
        name="collect",
    )(tiles_own, tiles_partner)


def prepare(own_x, partner_x, own_y, partner_y, dual_own, dual_partner, sizes):
    row_blocks, col_blocks, dim = sizes
    n_x, n_y = len(own_x), len(own_y)
    both = len(partner_y) > 0
    per_x = own_x[0].shape[0]
    per_y = own_y[0].shape[0] * (2 if both else 1)
    half_cols = col_blocks // 2
    all_rows = 2 * row_blocks
    chunks = TILE // LANES

    def kernel(*refs):
        refs = list(refs)

        def take(n):
            out = refs[:n]
            del refs[:n]
            return out

        xs, pxs, ys, pys = take(n_x), take(n_x), take(n_y), take(len(partner_y))
        d_own, d_partner = take(2)
        xp, yp, u0, wx, wy, nx, ny = take(7)
        row, col = lax.axis_index("row"), lax.axis_index("col")
        parity = lax.rem(row, 2)
        pair = lax.div(row, 2)

        def load(ref, b):
            points = jnp.concatenate([ref[b, j * dim : (j + 1) * dim, :] for j in range(chunks)], axis=1)
            base = chunks * dim
            weights = jnp.concatenate([ref[b, base + j : base + j + 1, :] for j in range(chunks)], axis=1)
            return points, weights

        def split(out, index, points):
            high = points.astype(jnp.bfloat16)
            low = (points - high.astype(jnp.float32)).astype(jnp.bfloat16)
            out[index, 0:dim, :] = high
            out[index, dim : 2 * dim, :] = low

        for group, (sources, duals) in enumerate(((xs, d_own), (pxs, d_partner))):
            side = parity if group == 0 else 1 - parity
            for d in range(n_x):
                for b in range(per_x):
                    local = (col ^ d) * per_x + b
                    index = side * row_blocks + local
                    points, weights = load(sources[d], b)
                    norm = jnp.sum(points * points, axis=0, keepdims=True)
                    split(xp, index, points * (2.0 * log2e / epsilon))
                    start = pl.multiple_of(local * TILE, TILE)
                    dual = duals[0:1, pl.ds(start, TILE)]
                    u0[pl.ds(index, 1), :] = log2e * weights + (dual - norm) * (log2e / epsilon)
                    wx[pl.ds(index, 1), :] = log2e * weights
                    nx[pl.ds(index, 1), :] = norm
        for d in range(n_y):
            place = pair ^ d
            for from_partner in range(2 if both else 1):
                source = (ys, pys)[from_partner][d]
                here = source.shape[0]
                for b in range(here):
                    index = place * per_y + b
                    if both:
                        index = index + (parity if from_partner == 0 else 1 - parity) * here
                    points, weights = load(source, b)
                    norm = jnp.sum(points * points, axis=0, keepdims=True)
                    split(yp, index, points)
                    wy[pl.ds(index, 1), :] = log2e * weights
                    ny[pl.ds(index, 1), :] = norm

    f32, bf16 = jnp.float32, jnp.bfloat16
    shape = jax.ShapeDtypeStruct
    rows, cols = (all_rows, TILE), (half_cols, TILE)
    return pl.pallas_call(
        kernel,
        out_shape=(
            shape((all_rows, 2 * dim, TILE), bf16),
            shape((half_cols, 2 * dim, TILE), bf16),
            shape(rows, f32),
            shape(rows, f32),
            shape(cols, f32),
            shape(rows, f32),
            shape(cols, f32),
        ),
        in_specs=[VM] * (2 * n_x + n_y + len(partner_y) + 2),
        out_specs=(VM,) * 7,
        compiler_params=PARAMS,
        name="prepare",
    )(*own_x, *partner_x, *own_y, *partner_y, dual_own, dual_partner)


def log_sum(parts):
    if len(parts) == 1:
        return parts[0]
    peak = functools.reduce(jnp.maximum, parts)
    total = functools.reduce(jnp.add, [jnp.exp2(part - peak) for part in parts])
    return peak + jnp.log2(total)


def half_step(from_points, to_points, weights, parts, guess, tiles, from_first, keep_total):
    m_blocks, width, _ = from_points.shape
    n_blocks = to_points.shape[0]
    dim = width // 2
    n_parts = len(parts)
    groups = TILE // 8
    guessed = guess is not None

    def kernel(*refs):
        tiles_ref, a_ref, b_ref, w_ref = refs[:4]
        part_refs = refs[4 : 4 + n_parts]
        rest = list(refs[4 + n_parts :])
        guess_ref = rest.pop(0) if guessed else None
        out_ref = rest.pop(0)
        total_ref = rest.pop(0) if keep_total else None
        lifts, drops, peaks, sums, s0, s1, p0, p1 = rest
        n = tiles_ref[0]

        def ends(k):
            code = tiles_ref[jnp.minimum(k, n) + 1]
            first, second = lax.shift_right_logical(code, SHIFT), code & (CODE - 1)
            return (first, second) if from_first else (second, first)


        if n_parts:
            total = log_sum([ref[...] for ref in part_refs])
            if keep_total:
                total_ref[...] = total
            lift = w_ref[...] - total
        else:
            lift = w_ref[...]
        place = lax.broadcasted_iota(jnp.int32, (BIAS, TILE), 0)

        def pieces(out, value, first, ones):
            high = value.astype(jnp.bfloat16).astype(jnp.float32)
            rest = value - high
            middle = rest.astype(jnp.bfloat16).astype(jnp.float32)
            low = rest - middle
            filler = jnp.where((place >= ones) & (place < ones + 3), 1.0, 0.0)
            for i in range(value.shape[0]):
                rows = filler
                for at, part in enumerate((high, middle, low)):
                    rows = jnp.where(place == first + at, part[i : i + 1, :], rows)
                out[i] = rows.astype(jnp.bfloat16)

        pieces(lifts, lift, 0, 3)
        plain = jnp.where(place < 3, 1.0, 0.0).astype(jnp.bfloat16)

        def doubled(ref, i, high_first):
            both = ref[i]
            if high_first:
                return [both[0:dim], both]
            return [both, both[0:dim]]

        def product(k, shifted, rows=TILE):
            m, c = ends(k)
            left = jnp.concatenate(doubled(a_ref, m, not from_first) + [lifts[m]], axis=0)[:, :rows]
            right = jnp.concatenate(doubled(b_ref, c, from_first) + [drops[c] if shifted else plain], axis=0)
            value = lax.dot_general(left, right, (((0,), (0,)), ((), ())), preferred_element_type=jnp.float32)
            return value.reshape(rows // 8, 8, TILE)

        def target(k):
            return jnp.where(k < n, ends(k)[1], n_blocks)

        def exact():
            peaks[...] = jnp.full(peaks.shape, lowest, jnp.float32)
            sums[...] = jnp.zeros(sums.shape, jnp.float32)

            def scores(k, score, peak):
                value = product(k, False)
                score[...] = value
                peak[...] = jnp.max(value, axis=0)

            def absorb(k, score, peak):
                c = target(k)
                before = peaks[c]
                after = jnp.maximum(before, peak[...])
                total = jnp.sum(jnp.exp2(score[...] - after[None]), axis=0)
                sums[c] = sums[c] * jnp.exp2(before - after) + total
                peaks[c] = after

            scores(0, s0, p0)

            def visit(step, carry):
                scores(2 * step + 1, s1, p1)
                absorb(2 * step, s0, p0)
                scores(2 * step + 2, s0, p0)
                absorb(2 * step + 1, s1, p1)
                return carry

            lax.fori_loop(0, lax.div(n + 1, 2), visit, 0)
            top = peaks[0:n_blocks]
            peak = jnp.max(top, axis=1)
            total = jnp.sum(sums[0:n_blocks] * jnp.exp2(top - peak[:, None, :]), axis=1)
            out_ref[...] = jnp.where(total > 0.0, peak + jnp.log2(total), lowest)

        batches = lax.div(n + UNROLL - 1, UNROLL)
        if guessed:
            shift = guess_ref[...]
        else:
            peaks[...] = jnp.full(peaks.shape, lowest, jnp.float32)

            def look(step, carry):
                found = []
                for u in range(UNROLL):
                    k = UNROLL * step + u
                    found.append((target(k), jnp.max(product(k, False, SAMPLE), axis=0)))
                for c, peak in found:
                    peaks[c] = jnp.maximum(peaks[c], peak)
                return carry

            lax.fori_loop(0, batches, look, 0)
            shift = jnp.max(peaks[0:n_blocks], axis=1) + MARGIN
        used = shift > 0.5 * lowest
        shift = jnp.where(used, shift, 0.0)
        pieces(drops, -shift, 3, 0)
        sums[...] = jnp.zeros(sums.shape, jnp.float32)

        def batch(start, size):
            found = []
            for k in range(size):
                value = product(start + k, True)
                found.append((target(start + k), jnp.sum(jnp.exp2(value), axis=0)))
            for c, total in found:
                sums[c] += total

        def visit(step, carry):
            batch(UNROLL * step, UNROLL)
            return carry

        even = lax.div(n + 1, 2) * 2
        full = lax.div(even, UNROLL)
        lax.fori_loop(0, full, visit, 0)
        done = full * UNROLL
        size = UNROLL // 2
        while size > 1:
            fits = even - done >= size
            pl.when(fits)(functools.partial(batch, done, size))
            done = jnp.where(fits, done + size, done)
            size //= 2
        total = jnp.sum(sums[0:n_blocks], axis=1)
        out_ref[...] = jnp.where(used, shift + jnp.log2(total), lowest)
        inside = (total > 2.0**-90) & (total < 2.0**120)
        outside = jnp.max(jnp.where(used & ~inside, 1.0, 0.0))
        pl.when(outside > 0.5)(exact)

    f32 = jnp.float32
    shape = jax.ShapeDtypeStruct
    out_shape = [shape((n_blocks, TILE), f32)] + ([shape((m_blocks, TILE), f32)] if keep_total else [])
    extra = (guess,) if guessed else ()
    return pl.pallas_call(
        kernel,
        out_shape=out_shape,
        in_specs=[SM] + [VM] * (3 + n_parts + len(extra)),
        out_specs=[VM] * len(out_shape),
        scratch_shapes=[
            pltpu.VMEM((m_blocks, BIAS, TILE), jnp.bfloat16),
            pltpu.VMEM((n_blocks, BIAS, TILE), jnp.bfloat16),
            pltpu.VMEM((n_blocks + 1, 8, TILE), f32),
            pltpu.VMEM((n_blocks + 1, 8, TILE), f32),
            pltpu.VMEM((groups, 8, TILE), f32),
            pltpu.VMEM((groups, 8, TILE), f32),
            pltpu.VMEM((8, TILE), f32),
            pltpu.VMEM((8, TILE), f32),
        ],
        compiler_params=PARAMS,
        name="column_step" if from_first else "row_step",
    )(tiles, from_points, to_points, weights, *parts, *extra)


def per_device(samples, sample_logw, references, reference_logw, dual_start, kept_tiles, tile_counts):
    n_row, n_col = lax.axis_size("row"), lax.axis_size("col")
    dim = samples.shape[1]
    own_row_blocks = samples.shape[0] // TILE
    own_col_blocks = references.shape[0] // TILE
    row_blocks, col_blocks = own_row_blocks * n_col, own_col_blocks * n_row
    chunks = TILE // LANES
    parity = lax.axis_index("row") % 2
    both = own_col_blocks % 2 == 0
    assert both or own_col_blocks == 1

    shape = jax.ShapeDtypeStruct
    depth = chunks * (dim + 1)
    kept = own_col_blocks // 2 if both else own_col_blocks
    packed_shapes = [shape((own_row_blocks, depth, LANES), jnp.float32)]
    packed_shapes += [shape((kept, depth, LANES), jnp.float32)] * (2 if both else 1)
    packed = pl.pallas_call(
        pack_kernel,
        out_shape=packed_shapes,
        in_specs=[HBM] * 4,
        out_specs=[VM] * len(packed_shapes),
        scratch_shapes=[
            pltpu.VMEM((own_row_blocks * chunks, LANES), jnp.float32),
            pltpu.VMEM((own_col_blocks * chunks, LANES), jnp.float32),
            pltpu.SemaphoreType.DMA((chunks * (own_row_blocks + own_col_blocks) + 2,)),
        ],
        compiler_params=PARAMS,
        name="pack",
    )(
        samples.T,
        sample_logw.reshape(-1, LANES),
        references.T,
        reference_logw.reshape(-1, LANES),
    )
    x_pack, y_keep = packed[0], packed[1]
    sends = [("col", d, x_pack) for d in range(n_col - 1, 0, -1)]
    plane = [("row", 2 * d, y_keep) for d in range(n_row // 2 - 1, 0, -1)]
    if both:
        plane += [("row", 2 * d + 1, packed[2]) for d in range(n_row // 2 - 1, -1, -1)]
    pace = max(1, len(plane) // len(sends))
    order = []
    while sends or plane:
        order += sends[:1] + plane[:pace]
        sends, plane = sends[1:], plane[pace:]
    tiles_own = jnp.concatenate([kept_tiles[0, 0], tile_counts[0]])
    order[2:2] = [("row", 0, tiles_own), ("row", -1, dual_start)]
    got = {}
    for axis, distance, value in order:
        got[axis, distance] = swap(value, axis, distance if distance > 0 else 1)
    own_y = [y_keep] + [got["row", 2 * d] for d in range(1, n_row // 2)]
    partner_y = [got["row", 2 * d + 1] for d in range(n_row // 2)] if both else []
    own_x = [x_pack] + [got["col", d] for d in range(1, n_col)]
    partner_x = [swap(part, "row", 1) for part in own_x]
    tiles_partner, dual_partner = got["row", 0], got["row", -1]
    tiles = collect_tiles(tiles_own, tiles_partner, row_blocks, col_blocks)
    xp, yp, start, wx, wy, nx, ny = prepare(
        own_x, partner_x, own_y, partner_y, dual_start, dual_partner, (row_blocks, col_blocks, dim)
    )

    row_parts = []
    col_guess = row_guess = None
    for turn in range(ITERS):
        last = turn == ITERS - 1
        (part,) = half_step(xp, yp, wx if turn else start, row_parts, col_guess, tiles, True, False)
        col_guess = part
        col_parts = [part] + [swap(part, "row", 2 * d) for d in range(1, n_row // 2)]
        part, *kept_total = half_step(yp, xp, wy, col_parts, row_guess, tiles, False, last)
        row_guess = part
        part = log_sum([part, swap(part, "row", 1)])
        row_parts = [part] + [swap(part, "col", d) for d in range(1, n_col)]

    own = [lax.dynamic_slice_in_dim(part, parity * row_blocks, row_blocks, 0) for part in row_parts]
    norms = lax.dynamic_slice_in_dim(nx, parity * row_blocks, row_blocks, 0)
    row_duals = norms - (epsilon * ln2) * log_sum(own)
    col_half = ny - (epsilon * ln2) * kept_total[0]
    col_other = swap(col_half, "row", 1)
    even = jnp.where(parity == 0, col_half, col_other)
    odd = jnp.where(parity == 0, col_other, col_half)
    col_duals = jnp.stack([even, odd], axis=1)
    return (row_duals.reshape(1, -1), col_duals.reshape(1, -1))


def solution(mesh):
    return jax.shard_map(
        per_device,
        mesh=mesh,
        in_specs=(
            P(("row", "col"), None),
            P(("row", "col")),
            P(("row", "col"), None),
            P(("row", "col")),
            P("row", None),
            P("row", "col", None),
            P("row", "col"),
        ),
        out_specs=(P("row", None), P("col", None)),
        check_vma=False,
    )
```

```python
import functools
import math

import jax
import jax.numpy as jnp
from jax import lax
from jax.experimental import pallas as pl
from jax.experimental.pallas import tpu as pltpu
from jax.sharding import PartitionSpec as P


TILE = 512
ITERS = 3
LANES = 128
BIAS = 16
SHIFT = 12
CODE = 1 << SHIFT
UNROLL = 8
SAMPLE = 128
MARGIN = 80.0

lowest = -1e30
epsilon = 0.1
log2e = math.log2(math.e)
ln2 = math.log(2.0)


VM = pl.BlockSpec(memory_space=pltpu.VMEM)
SM = pl.BlockSpec(memory_space=pltpu.SMEM)
PARAMS = pltpu.CompilerParams(vmem_limit_bytes=24 * 1024 * 1024)


def swap(value, axis, distance):
    pairs = [(i, i ^ distance) for i in range(lax.axis_size(axis))]
    return jax.tree.map(lambda part: lax.ppermute(part, axis, pairs), value)


def pack_kernel(points_ref, weights_ref, *outs):
    dim = points_ref.shape[0]
    chunks = TILE // LANES

    def put(out, b, block):
        for j in range(chunks):
            start = pl.multiple_of(block * TILE + j * LANES, LANES)
            out[b, j * dim : (j + 1) * dim, :] = points_ref[:, pl.ds(start, LANES)]
        out[b, chunks * dim : chunks * (dim + 1), :] = weights_ref[pl.ds(block * chunks, chunks), :]

    x_ref, keep_ref, *send_refs = outs
    first = x_ref.shape[0]
    for b in range(first):
        put(x_ref, b, b)
    if send_refs:
        parity = lax.rem(lax.axis_index("row"), 2)
        for b in range(keep_ref.shape[0]):
            put(send_refs[0], b, first + 2 * b + 1 - parity)
            put(keep_ref, b, first + 2 * b + parity)
    else:
        for b in range(keep_ref.shape[0]):
            put(keep_ref, b, first + b)


def collect_tiles(tiles_own, tiles_partner, row_blocks, col_blocks):
    slots = tiles_own.shape[0] - 1

    firsts = (2 * slots + 2, 2 * slots + 2 + 2 * row_blocks + 2)

    def kernel(t_own, t_partner, found, seen_row, seen_col):
        parity = lax.rem(lax.axis_index("row"), 2)
        for seen in (seen_row, seen_col):
            for i in range(seen.shape[0]):
                seen[i] = 0

        def collect(ref, side, filled):
            def visit(k, filled):
                n, rows, cols = filled
                tile = ref[k]
                r, c = side * row_blocks + lax.div(tile, col_blocks), lax.rem(tile, col_blocks)
                mine = (lax.rem(c, 2) == parity).astype(jnp.int32)
                c = lax.div(c, 2)
                code = r * CODE + c
                found[n] = code
                new_row, new_col = mine * (1 - seen_row[r]), mine * (1 - seen_col[c])
                found[rows] = code
                found[cols] = code
                seen_row[r] = seen_row[r] | mine
                seen_col[c] = seen_col[c] | mine
                return (n + mine, rows + new_row, cols + new_col)

            return lax.fori_loop(0, ref[slots], visit, filled)

        filled = (jnp.int32(1), jnp.int32(firsts[0] + 1), jnp.int32(firsts[1] + 1))
        filled = collect(t_own, parity, filled)
        filled = collect(t_partner, 1 - parity, filled)
        for at, end in zip((0,) + firsts, filled):
            found[at] = end - at - 1
            found[end] = 0

    tiles = pl.pallas_call(
        kernel,
        out_shape=jax.ShapeDtypeStruct((firsts[1] + col_blocks // 2 + 2,), jnp.int32),
        in_specs=[SM] * 2,
        out_specs=SM,
        scratch_shapes=[pltpu.SMEM((2 * row_blocks,), jnp.int32), pltpu.SMEM((col_blocks // 2,), jnp.int32)],
        compiler_params=PARAMS,
        name="collect",
    )(tiles_own, tiles_partner)
    return tiles, firsts


def prepare(own_x, partner_x, own_y, partner_y, dual_own, dual_partner, sizes):
    row_blocks, col_blocks, dim = sizes
    n_x, n_y = len(own_x), len(own_y)
    both = len(partner_y) > 0
    per_x = own_x[0].shape[0]
    per_y = own_y[0].shape[0] * (2 if both else 1)
    half_cols = col_blocks // 2
    all_rows = 2 * row_blocks
    chunks = TILE // LANES

    def kernel(*refs):
        refs = list(refs)

        def take(n):
            out = refs[:n]
            del refs[:n]
            return out

        xs, pxs, ys, pys = take(n_x), take(n_x), take(n_y), take(len(partner_y))
        d_own, d_partner = take(2)
        xp, yp, u0, wx, wy, nx, ny = take(7)
        row, col = lax.axis_index("row"), lax.axis_index("col")
        parity = lax.rem(row, 2)
        pair = lax.div(row, 2)

        def load(ref, b):
            points = jnp.concatenate([ref[b, j * dim : (j + 1) * dim, :] for j in range(chunks)], axis=1)
            base = chunks * dim
            weights = jnp.concatenate([ref[b, base + j : base + j + 1, :] for j in range(chunks)], axis=1)
            return points, weights

        def split(out, index, points):
            high = points.astype(jnp.bfloat16)
            low = (points - high.astype(jnp.float32)).astype(jnp.bfloat16)
            out[index, 0:dim, :] = high
            out[index, dim : 2 * dim, :] = low

        for group, (sources, duals) in enumerate(((xs, d_own), (pxs, d_partner))):
            side = parity if group == 0 else 1 - parity
            for d in range(n_x):
                for b in range(per_x):
                    local = (col ^ d) * per_x + b
                    index = side * row_blocks + local
                    points, weights = load(sources[d], b)
                    norm = jnp.sum(points * points, axis=0, keepdims=True)
                    split(xp, index, points * (2.0 * log2e / epsilon))
                    start = pl.multiple_of(local * TILE, TILE)
                    dual = duals[0:1, pl.ds(start, TILE)]
                    u0[pl.ds(index, 1), :] = log2e * weights + (dual - norm) * (log2e / epsilon)
                    wx[pl.ds(index, 1), :] = log2e * weights
                    nx[pl.ds(index, 1), :] = norm
        for d in range(n_y):
            place = pair ^ d
            for from_partner in range(2 if both else 1):
                source = (ys, pys)[from_partner][d]
                here = source.shape[0]
                for b in range(here):
                    index = place * per_y + b
                    if both:
                        index = index + (parity if from_partner == 0 else 1 - parity) * here
                    points, weights = load(source, b)
                    norm = jnp.sum(points * points, axis=0, keepdims=True)
                    split(yp, index, points)
                    wy[pl.ds(index, 1), :] = log2e * weights
                    ny[pl.ds(index, 1), :] = norm

    f32, bf16 = jnp.float32, jnp.bfloat16
    shape = jax.ShapeDtypeStruct
    rows, cols = (all_rows, TILE), (half_cols, TILE)
    return pl.pallas_call(
        kernel,
        out_shape=(
            shape((all_rows, 2 * dim, TILE), bf16),
            shape((half_cols, 2 * dim, TILE), bf16),
            shape(rows, f32),
            shape(rows, f32),
            shape(cols, f32),
            shape(rows, f32),
            shape(cols, f32),
        ),
        in_specs=[VM] * (2 * n_x + n_y + len(partner_y) + 2),
        out_specs=(VM,) * 7,
        compiler_params=PARAMS,
        name="prepare",
    )(*own_x, *partner_x, *own_y, *partner_y, dual_own, dual_partner)


def log_sum(parts):
    if len(parts) == 1:
        return parts[0]
    peak = functools.reduce(jnp.maximum, parts)
    total = functools.reduce(jnp.add, [jnp.exp2(part - peak) for part in parts])
    return peak + jnp.log2(total)


def half_step(from_points, to_points, weights, parts, guess, tiles, first, from_first, keep_total):
    m_blocks, width, _ = from_points.shape
    n_blocks = to_points.shape[0]
    dim = width // 2
    n_parts = len(parts)
    groups = TILE // 8
    guessed = guess is not None

    def kernel(*refs):
        listed_ref, a_ref, b_ref, w_ref = refs[:4]
        part_refs = refs[4 : 4 + n_parts]
        rest = list(refs[4 + n_parts :])
        guess_ref = rest.pop(0) if guessed else None
        out_ref = rest.pop(0)
        total_ref = rest.pop(0) if keep_total else None
        lifts, drops, peaks, sums, s0, s1, p0, p1, tiles_ref, arrived = rest
        listing = pltpu.make_async_copy(listed_ref, tiles_ref, arrived)
        listing.start()

        def ends(k, base=0):
            code = tiles_ref[base + jnp.minimum(k, tiles_ref[base]) + 1]
            above, below = lax.shift_right_logical(code, SHIFT), code & (CODE - 1)
            return (above, below) if from_first else (below, above)


        if n_parts:
            total = log_sum([ref[...] for ref in part_refs])
            if keep_total:
                total_ref[...] = total
            lift = w_ref[...] - total
        else:
            lift = w_ref[...]
        place = lax.broadcasted_iota(jnp.int32, (BIAS, TILE), 0)

        def pieces(out, value, first, ones):
            high = value.astype(jnp.bfloat16).astype(jnp.float32)
            rest = value - high
            middle = rest.astype(jnp.bfloat16).astype(jnp.float32)
            low = rest - middle
            filler = jnp.where((place >= ones) & (place < ones + 3), 1.0, 0.0)
            for i in range(value.shape[0]):
                rows = filler
                for at, part in enumerate((high, middle, low)):
                    rows = jnp.where(place == first + at, part[i : i + 1, :], rows)
                out[i] = rows.astype(jnp.bfloat16)

        pieces(lifts, lift, 0, 3)
        plain = jnp.where(place < 3, 1.0, 0.0).astype(jnp.bfloat16)
        if guessed:
            shift = guess_ref[...]
            used = shift > 0.5 * lowest
            shift = jnp.where(used, shift, 0.0)
            pieces(drops, -shift, 3, 0)
        sums[...] = jnp.zeros(sums.shape, jnp.float32)
        listing.wait()
        n = tiles_ref[0]

        def doubled(ref, i, high_first):
            both = ref[i]
            if high_first:
                return [both[0:dim], both]
            return [both, both[0:dim]]

        def product(k, shifted, rows=TILE, base=0):
            m, c = ends(k, base)
            left = jnp.concatenate(doubled(a_ref, m, not from_first) + [lifts[m]], axis=0)[:, :rows]
            right = jnp.concatenate(doubled(b_ref, c, from_first) + [drops[c] if shifted else plain], axis=0)
            value = lax.dot_general(left, right, (((0,), (0,)), ((), ())), preferred_element_type=jnp.float32)
            return value.reshape(rows // 8, 8, TILE)

        def target(k, base=0):
            return jnp.where(k < tiles_ref[base], ends(k, base)[1], n_blocks)

        def exact():
            peaks[...] = jnp.full(peaks.shape, lowest, jnp.float32)
            sums[...] = jnp.zeros(sums.shape, jnp.float32)

            def scores(k, score, peak):
                value = product(k, False)
                score[...] = value
                peak[...] = jnp.max(value, axis=0)

            def absorb(k, score, peak):
                c = target(k)
                before = peaks[c]
                after = jnp.maximum(before, peak[...])
                total = jnp.sum(jnp.exp2(score[...] - after[None]), axis=0)
                sums[c] = sums[c] * jnp.exp2(before - after) + total
                peaks[c] = after

            scores(0, s0, p0)

            def visit(step, carry):
                scores(2 * step + 1, s1, p1)
                absorb(2 * step, s0, p0)
                scores(2 * step + 2, s0, p0)
                absorb(2 * step + 1, s1, p1)
                return carry

            lax.fori_loop(0, lax.div(n + 1, 2), visit, 0)
            top = peaks[0:n_blocks]
            peak = jnp.max(top, axis=1)
            total = jnp.sum(sums[0:n_blocks] * jnp.exp2(top - peak[:, None, :]), axis=1)
            out_ref[...] = jnp.where(total > 0.0, peak + jnp.log2(total), lowest)

        if not guessed:
            peaks[...] = jnp.full(peaks.shape, lowest, jnp.float32)

            def look(step, carry):
                found = []
                for u in range(UNROLL):
                    k = UNROLL * step + u
                    found.append((target(k, first), jnp.max(product(k, False, SAMPLE, first), axis=0)))
                for c, peak in found:
                    peaks[c] = jnp.maximum(peaks[c], peak)
                return carry

            lax.fori_loop(0, lax.div(tiles_ref[first] + UNROLL - 1, UNROLL), look, 0)
            shift = jnp.max(peaks[0:n_blocks], axis=1) + MARGIN
            used = shift > 0.5 * lowest
            shift = jnp.where(used, shift, 0.0)
            pieces(drops, -shift, 3, 0)

        def batch(start, size):
            found = []
            for k in range(size):
                value = product(start + k, True)
                found.append((target(start + k), jnp.sum(jnp.exp2(value), axis=0)))
            for c, total in found:
                sums[c] += total

        def visit(step, carry):
            batch(UNROLL * step, UNROLL)
            return carry

        even = lax.div(n + 1, 2) * 2
        full = lax.div(even, UNROLL)
        lax.fori_loop(0, full, visit, 0)
        done = full * UNROLL
        size = UNROLL // 2
        while size > 1:
            fits = even - done >= size
            pl.when(fits)(functools.partial(batch, done, size))
            done = jnp.where(fits, done + size, done)
            size //= 2
        total = jnp.sum(sums[0:n_blocks], axis=1)
        out_ref[...] = jnp.where(used, shift + jnp.log2(total), lowest)
        inside = (total > 2.0**-90) & (total < 2.0**120)
        outside = jnp.max(jnp.where(used & ~inside, 1.0, 0.0))
        pl.when(outside > 0.5)(exact)

    f32 = jnp.float32
    shape = jax.ShapeDtypeStruct
    out_shape = [shape((n_blocks, TILE), f32)] + ([shape((m_blocks, TILE), f32)] if keep_total else [])
    extra = (guess,) if guessed else ()
    return pl.pallas_call(
        kernel,
        out_shape=out_shape,
        in_specs=[VM] * (4 + n_parts + len(extra)),
        out_specs=[VM] * len(out_shape),
        scratch_shapes=[
            pltpu.VMEM((m_blocks, BIAS, TILE), jnp.bfloat16),
            pltpu.VMEM((n_blocks, BIAS, TILE), jnp.bfloat16),
            pltpu.VMEM((n_blocks + 1, 8, TILE), f32),
            pltpu.VMEM((n_blocks + 1, 8, TILE), f32),
            pltpu.VMEM((groups, 8, TILE), f32),
            pltpu.VMEM((groups, 8, TILE), f32),
            pltpu.VMEM((8, TILE), f32),
            pltpu.VMEM((8, TILE), f32),
            pltpu.SMEM(tiles.shape, jnp.int32),
            pltpu.SemaphoreType.DMA(()),
        ],
        compiler_params=PARAMS,
        name="column_step" if from_first else "row_step",
    )(tiles, from_points, to_points, weights, *parts, *extra)


def per_device(samples, sample_logw, references, reference_logw, dual_start, kept_tiles, tile_counts):
    n_row, n_col = lax.axis_size("row"), lax.axis_size("col")
    dim = samples.shape[1]
    own_row_blocks = samples.shape[0] // TILE
    own_col_blocks = references.shape[0] // TILE
    row_blocks, col_blocks = own_row_blocks * n_col, own_col_blocks * n_row
    chunks = TILE // LANES
    parity = lax.axis_index("row") % 2
    both = own_col_blocks % 2 == 0
    assert both or own_col_blocks == 1

    shape = jax.ShapeDtypeStruct
    depth = chunks * (dim + 1)
    kept = own_col_blocks // 2 if both else own_col_blocks
    packed_shapes = [shape((own_row_blocks, depth, LANES), jnp.float32)]
    packed_shapes += [shape((kept, depth, LANES), jnp.float32)] * (2 if both else 1)
    packed = pl.pallas_call(
        pack_kernel,
        out_shape=packed_shapes,
        in_specs=[VM] * 2,
        out_specs=[VM] * len(packed_shapes),
        compiler_params=PARAMS,
        name="pack",
    )(
        jnp.concatenate([samples.T, references.T], axis=1),
        jnp.concatenate([sample_logw, reference_logw]).reshape(-1, LANES),
    )
    x_pack, y_keep = packed[0], packed[1]
    sends = [("col", d, x_pack) for d in range(n_col - 1, 0, -1)]
    plane = [("row", 2 * d, y_keep) for d in range(n_row // 2 - 1, 0, -1)]
    if both:
        plane += [("row", 2 * d + 1, packed[2]) for d in range(n_row // 2 - 1, -1, -1)]
    pace = max(1, len(plane) // len(sends))
    order = []
    while sends or plane:
        order += sends[:1] + plane[:pace]
        sends, plane = sends[1:], plane[pace:]
    tiles_own = jnp.concatenate([kept_tiles[0, 0], tile_counts[0]])
    order[7:7] = [("row", 0, tiles_own), ("row", -1, dual_start)]
    got = {}
    for axis, distance, value in order:
        got[axis, distance] = swap(value, axis, distance if distance > 0 else 1)
    own_y = [y_keep] + [got["row", 2 * d] for d in range(1, n_row // 2)]
    partner_y = [got["row", 2 * d + 1] for d in range(n_row // 2)] if both else []
    own_x = [x_pack] + [got["col", d] for d in range(1, n_col)]
    partner_x = [swap(part, "row", 1) for part in own_x]
    tiles_partner, dual_partner = got["row", 0], got["row", -1]
    tiles, firsts = collect_tiles(tiles_own, tiles_partner, row_blocks, col_blocks)
    xp, yp, start, wx, wy, nx, ny = prepare(
        own_x, partner_x, own_y, partner_y, dual_start, dual_partner, (row_blocks, col_blocks, dim)
    )

    row_parts = []
    col_guess = row_guess = None
    for turn in range(ITERS):
        last = turn == ITERS - 1
        (part,) = half_step(xp, yp, wx if turn else start, row_parts, col_guess, tiles, firsts[1], True, False)
        col_guess = part
        col_parts = [part] + [swap(part, "row", 2 * d) for d in range(1, n_row // 2)]
        part, *kept_total = half_step(yp, xp, wy, col_parts, row_guess, tiles, firsts[0], False, last)
        row_guess = part
        if last:
            mine, other = (
                lax.dynamic_slice_in_dim(part, side * row_blocks, row_blocks, 0) for side in (parity, 1 - parity)
            )
        else:
            mine = other = part
        part = log_sum([mine, swap(other, "row", 1)])
        row_parts = [part] + [swap(part, "col", d) for d in range(1, n_col)]

    norms = lax.dynamic_slice_in_dim(nx, parity * row_blocks, row_blocks, 0)

    def finish(norms_ref, *refs):
        *parts, out = refs
        duals = norms_ref[...] - (epsilon * ln2) * log_sum([part[...] for part in parts])
        for b in range(row_blocks):
            out[0:1, b * TILE : (b + 1) * TILE] = duals[b : b + 1, :]

    row_duals = pl.pallas_call(
        finish,
        out_shape=shape(dual_start.shape, jnp.float32),
        in_specs=[VM] * (1 + n_col),
        out_specs=VM,
        compiler_params=PARAMS,
        name="finish",
    )(norms, *row_parts)
    col_half = ny - (epsilon * ln2) * kept_total[0]
    col_other = swap(col_half, "row", 1)
    even = jnp.where(parity == 0, col_half, col_other)
    odd = jnp.where(parity == 0, col_other, col_half)
    col_duals = jnp.stack([even, odd], axis=1)
    return (row_duals, col_duals.reshape(1, -1))


def solution(mesh):
    return jax.shard_map(
        per_device,
        mesh=mesh,
        in_specs=(
            P(("row", "col"), None),
            P(("row", "col")),
            P(("row", "col"), None),
            P(("row", "col")),
            P("row", None),
            P("row", "col", None),
            P("row", "col"),
        ),
        out_specs=(P("row", None), P("col", None)),
        check_vma=False,
    )
```

```python
import functools
import math

import jax
import jax.numpy as jnp
from jax import lax
from jax.experimental import pallas as pl
from jax.experimental.pallas import tpu as pltpu
from jax.sharding import PartitionSpec as P


TILE = 512
ITERS = 3
LANES = 128
BIAS = 16
SHIFT = 12
CODE = 1 << SHIFT
UNROLL = 8
SAMPLE = 128
MARGIN = 80.0

lowest = -1e30
epsilon = 0.1
log2e = math.log2(math.e)
ln2 = math.log(2.0)


VM = pl.BlockSpec(memory_space=pltpu.VMEM)
SM = pl.BlockSpec(memory_space=pltpu.SMEM)
PARAMS = pltpu.CompilerParams(vmem_limit_bytes=24 * 1024 * 1024)


def swap(value, axis, distance):
    pairs = [(i, i ^ distance) for i in range(lax.axis_size(axis))]
    return jax.tree.map(lambda part: lax.ppermute(part, axis, pairs), value)


def pack_kernel(points_ref, weights_ref, *outs):
    dim = points_ref.shape[0]
    chunks = TILE // LANES

    def put(out, b, block):
        for j in range(chunks):
            start = pl.multiple_of(block * TILE + j * LANES, LANES)
            out[b, j * dim : (j + 1) * dim, :] = points_ref[:, pl.ds(start, LANES)]
        out[b, chunks * dim : chunks * (dim + 1), :] = weights_ref[pl.ds(block * chunks, chunks), :]

    x_ref, keep_ref, *send_refs = outs
    first = x_ref.shape[0]
    for b in range(first):
        put(x_ref, b, b)
    if send_refs:
        parity = lax.rem(lax.axis_index("row"), 2)
        for b in range(keep_ref.shape[0]):
            put(send_refs[0], b, first + 2 * b + 1 - parity)
            put(keep_ref, b, first + 2 * b + parity)
    else:
        for b in range(keep_ref.shape[0]):
            put(keep_ref, b, first + b)


def collect_tiles(tiles_own, tiles_partner, row_blocks, col_blocks):
    slots = tiles_own.shape[0] - 1

    firsts = (2 * slots + 2, 2 * slots + 2 + 2 * row_blocks + 2)

    def kernel(t_own, t_partner, found, seen_row, seen_col):
        parity = lax.rem(lax.axis_index("row"), 2)
        for seen in (seen_row, seen_col):
            for i in range(seen.shape[0]):
                seen[i] = 0

        bits = col_blocks.bit_length() - 1
        if col_blocks == 1 << bits:
            above, below = lambda tile: lax.shift_right_logical(tile, bits), lambda tile: tile & (col_blocks - 1)
        else:
            above, below = lambda tile: lax.div(tile, col_blocks), lambda tile: lax.rem(tile, col_blocks)

        def collect(ref, side, filled):
            def visit(k, filled):
                n, rows, cols = filled
                tile = ref[k]
                r, c = side * row_blocks + above(tile), below(tile)
                mine = 1 - ((c ^ parity) & 1)
                c = lax.shift_right_logical(c, 1)
                code = r * CODE + c
                found[n] = code
                new_row, new_col = mine * (1 - seen_row[r]), mine * (1 - seen_col[c])
                found[rows] = code
                found[cols] = code
                seen_row[r] = seen_row[r] | mine
                seen_col[c] = seen_col[c] | mine
                return (n + mine, rows + new_row, cols + new_col)

            return lax.fori_loop(0, ref[slots], visit, filled)

        filled = (jnp.int32(1), jnp.int32(firsts[0] + 1), jnp.int32(firsts[1] + 1))
        filled = collect(t_own, parity, filled)
        filled = collect(t_partner, 1 - parity, filled)
        for at, end in zip((0,) + firsts, filled):
            found[at] = end - at - 1
            found[end] = 0

    tiles = pl.pallas_call(
        kernel,
        out_shape=jax.ShapeDtypeStruct((firsts[1] + col_blocks // 2 + 2,), jnp.int32),
        in_specs=[SM] * 2,
        out_specs=SM,
        scratch_shapes=[pltpu.SMEM((2 * row_blocks,), jnp.int32), pltpu.SMEM((col_blocks // 2,), jnp.int32)],
        compiler_params=PARAMS,
        name="collect",
    )(tiles_own, tiles_partner)
    return tiles, firsts


def prepare(own_x, partner_x, own_y, partner_y, dual_own, dual_partner, sizes):
    row_blocks, col_blocks, dim = sizes
    n_x, n_y = len(own_x), len(own_y)
    both = len(partner_y) > 0
    per_x = own_x[0].shape[0]
    per_y = own_y[0].shape[0] * (2 if both else 1)
    half_cols = col_blocks // 2
    all_rows = 2 * row_blocks
    chunks = TILE // LANES

    def kernel(*refs):
        refs = list(refs)

        def take(n):
            out = refs[:n]
            del refs[:n]
            return out

        xs, pxs, ys, pys = take(n_x), take(n_x), take(n_y), take(len(partner_y))
        d_own, d_partner = take(2)
        xp, yp, u0, wx, wy, nx, ny = take(7)
        row, col = lax.axis_index("row"), lax.axis_index("col")
        parity = lax.rem(row, 2)
        pair = lax.div(row, 2)

        def load(ref, b):
            points = jnp.concatenate([ref[b, j * dim : (j + 1) * dim, :] for j in range(chunks)], axis=1)
            base = chunks * dim
            weights = jnp.concatenate([ref[b, base + j : base + j + 1, :] for j in range(chunks)], axis=1)
            return points, weights

        def split(out, index, points):
            high = points.astype(jnp.bfloat16)
            low = (points - high.astype(jnp.float32)).astype(jnp.bfloat16)
            out[index, 0:dim, :] = high
            out[index, dim : 2 * dim, :] = low

        for group, (sources, duals) in enumerate(((xs, d_own), (pxs, d_partner))):
            side = parity if group == 0 else 1 - parity
            for d in range(n_x):
                for b in range(per_x):
                    local = (col ^ d) * per_x + b
                    index = side * row_blocks + local
                    points, weights = load(sources[d], b)
                    norm = jnp.sum(points * points, axis=0, keepdims=True)
                    split(xp, index, points * (2.0 * log2e / epsilon))
                    start = pl.multiple_of(local * TILE, TILE)
                    dual = duals[0:1, pl.ds(start, TILE)]
                    u0[pl.ds(index, 1), :] = log2e * weights + (dual - norm) * (log2e / epsilon)
                    wx[pl.ds(index, 1), :] = log2e * weights
                    nx[pl.ds(index, 1), :] = norm
        for d in range(n_y):
            place = pair ^ d
            for from_partner in range(2 if both else 1):
                source = (ys, pys)[from_partner][d]
                here = source.shape[0]
                for b in range(here):
                    index = place * per_y + b
                    if both:
                        index = index + (parity if from_partner == 0 else 1 - parity) * here
                    points, weights = load(source, b)
                    norm = jnp.sum(points * points, axis=0, keepdims=True)
                    split(yp, index, points)
                    wy[pl.ds(index, 1), :] = log2e * weights
                    ny[pl.ds(index, 1), :] = norm

    f32, bf16 = jnp.float32, jnp.bfloat16
    shape = jax.ShapeDtypeStruct
    rows, cols = (all_rows, TILE), (half_cols, TILE)
    return pl.pallas_call(
        kernel,
        out_shape=(
            shape((all_rows, 2 * dim, TILE), bf16),
            shape((half_cols, 2 * dim, TILE), bf16),
            shape(rows, f32),
            shape(rows, f32),
            shape(cols, f32),
            shape(rows, f32),
            shape(cols, f32),
        ),
        in_specs=[VM] * (2 * n_x + n_y + len(partner_y) + 2),
        out_specs=(VM,) * 7,
        compiler_params=PARAMS,
        name="prepare",
    )(*own_x, *partner_x, *own_y, *partner_y, dual_own, dual_partner)


def log_sum(parts):
    if len(parts) == 1:
        return parts[0]
    peak = functools.reduce(jnp.maximum, parts)
    total = functools.reduce(jnp.add, [jnp.exp2(part - peak) for part in parts])
    return peak + jnp.log2(total)


def half_step(from_points, to_points, weights, parts, guess, tiles, first, from_first, keep_total):
    m_blocks, width, _ = from_points.shape
    n_blocks = to_points.shape[0]
    dim = width // 2
    n_parts = len(parts)
    groups = TILE // 8
    guessed = guess is not None

    def kernel(*refs):
        listed_ref, a_ref, b_ref, w_ref = refs[:4]
        part_refs = refs[4 : 4 + n_parts]
        rest = list(refs[4 + n_parts :])
        guess_ref = rest.pop(0) if guessed else None
        out_ref = rest.pop(0)
        total_ref = rest.pop(0) if keep_total else None
        lifts, drops, peaks, sums, s0, s1, p0, p1, tiles_ref, arrived = rest
        listing = pltpu.make_async_copy(listed_ref, tiles_ref, arrived)
        listing.start()

        def ends(k, base=0):
            code = tiles_ref[base + jnp.minimum(k, tiles_ref[base]) + 1]
            above, below = lax.shift_right_logical(code, SHIFT), code & (CODE - 1)
            return (above, below) if from_first else (below, above)


        if n_parts:
            total = log_sum([ref[...] for ref in part_refs])
            if keep_total:
                total_ref[...] = total
            lift = w_ref[...] - total
        else:
            lift = w_ref[...]
        place = lax.broadcasted_iota(jnp.int32, (BIAS, TILE), 0)

        def pieces(out, value, first, ones):
            high = value.astype(jnp.bfloat16).astype(jnp.float32)
            rest = value - high
            middle = rest.astype(jnp.bfloat16).astype(jnp.float32)
            low = rest - middle
            filler = jnp.where((place >= ones) & (place < ones + 3), 1.0, 0.0)
            for i in range(value.shape[0]):
                rows = filler
                for at, part in enumerate((high, middle, low)):
                    rows = jnp.where(place == first + at, part[i : i + 1, :], rows)
                out[i] = rows.astype(jnp.bfloat16)

        pieces(lifts, lift, 0, 3)
        plain = jnp.where(place < 3, 1.0, 0.0).astype(jnp.bfloat16)
        if guessed:
            shift = guess_ref[...]
            used = shift > 0.5 * lowest
            shift = jnp.where(used, shift, 0.0)
            pieces(drops, -shift, 3, 0)
        sums[...] = jnp.zeros(sums.shape, jnp.float32)
        listing.wait()
        n = tiles_ref[0]

        def doubled(ref, i, high_first):
            both = ref[i]
            if high_first:
                return [both[0:dim], both]
            return [both, both[0:dim]]

        def product(k, shifted, rows=TILE, base=0):
            m, c = ends(k, base)
            left = jnp.concatenate(doubled(a_ref, m, not from_first) + [lifts[m]], axis=0)[:, :rows]
            right = jnp.concatenate(doubled(b_ref, c, from_first) + [drops[c] if shifted else plain], axis=0)
            value = lax.dot_general(left, right, (((0,), (0,)), ((), ())), preferred_element_type=jnp.float32)
            return value.reshape(rows // 8, 8, TILE)

        def target(k, base=0):
            return jnp.where(k < tiles_ref[base], ends(k, base)[1], n_blocks)

        def exact():
            peaks[...] = jnp.full(peaks.shape, lowest, jnp.float32)
            sums[...] = jnp.zeros(sums.shape, jnp.float32)

            def scores(k, score, peak):
                value = product(k, False)
                score[...] = value
                peak[...] = jnp.max(value, axis=0)

            def absorb(k, score, peak):
                c = target(k)
                before = peaks[c]
                after = jnp.maximum(before, peak[...])
                total = jnp.sum(jnp.exp2(score[...] - after[None]), axis=0)
                sums[c] = sums[c] * jnp.exp2(before - after) + total
                peaks[c] = after

            scores(0, s0, p0)

            def visit(step, carry):
                scores(2 * step + 1, s1, p1)
                absorb(2 * step, s0, p0)
                scores(2 * step + 2, s0, p0)
                absorb(2 * step + 1, s1, p1)
                return carry

            lax.fori_loop(0, lax.div(n + 1, 2), visit, 0)
            top = peaks[0:n_blocks]
            peak = jnp.max(top, axis=1)
            total = jnp.sum(sums[0:n_blocks] * jnp.exp2(top - peak[:, None, :]), axis=1)
            out_ref[...] = jnp.where(total > 0.0, peak + jnp.log2(total), lowest)

        if not guessed:
            peaks[...] = jnp.full(peaks.shape, lowest, jnp.float32)

            def look(step, carry):
                found = []
                for u in range(UNROLL):
                    k = UNROLL * step + u
                    found.append((target(k, first), jnp.max(product(k, False, SAMPLE, first), axis=0)))
                for c, peak in found:
                    peaks[c] = jnp.maximum(peaks[c], peak)
                return carry

            lax.fori_loop(0, lax.div(tiles_ref[first] + UNROLL - 1, UNROLL), look, 0)
            shift = jnp.max(peaks[0:n_blocks], axis=1) + MARGIN
            used = shift > 0.5 * lowest
            shift = jnp.where(used, shift, 0.0)
            pieces(drops, -shift, 3, 0)

        def batch(start, size):
            found = []
            for k in range(size):
                value = product(start + k, True)
                found.append((target(start + k), jnp.sum(jnp.exp2(value), axis=0)))
            for c, total in found:
                sums[c] += total

        def visit(step, carry):
            batch(UNROLL * step, UNROLL)
            return carry

        even = lax.div(n + 1, 2) * 2
        full = lax.div(even, UNROLL)
        lax.fori_loop(0, full, visit, 0)
        done = full * UNROLL
        size = UNROLL // 2
        while size > 1:
            fits = even - done >= size
            pl.when(fits)(functools.partial(batch, done, size))
            done = jnp.where(fits, done + size, done)
            size //= 2
        total = jnp.sum(sums[0:n_blocks], axis=1)
        out_ref[...] = jnp.where(used, shift + jnp.log2(total), lowest)
        inside = (total > 2.0**-90) & (total < 2.0**120)
        outside = jnp.max(jnp.where(used & ~inside, 1.0, 0.0))
        pl.when(outside > 0.5)(exact)

    f32 = jnp.float32
    shape = jax.ShapeDtypeStruct
    out_shape = [shape((n_blocks, TILE), f32)] + ([shape((m_blocks, TILE), f32)] if keep_total else [])
    extra = (guess,) if guessed else ()
    return pl.pallas_call(
        kernel,
        out_shape=out_shape,
        in_specs=[VM] * (4 + n_parts + len(extra)),
        out_specs=[VM] * len(out_shape),
        scratch_shapes=[
            pltpu.VMEM((m_blocks, BIAS, TILE), jnp.bfloat16),
            pltpu.VMEM((n_blocks, BIAS, TILE), jnp.bfloat16),
            pltpu.VMEM((n_blocks + 1, 8, TILE), f32),
            pltpu.VMEM((n_blocks + 1, 8, TILE), f32),
            pltpu.VMEM((groups, 8, TILE), f32),
            pltpu.VMEM((groups, 8, TILE), f32),
            pltpu.VMEM((8, TILE), f32),
            pltpu.VMEM((8, TILE), f32),
            pltpu.SMEM(tiles.shape, jnp.int32),
            pltpu.SemaphoreType.DMA(()),
        ],
        compiler_params=PARAMS,
        name="column_step" if from_first else "row_step",
    )(tiles, from_points, to_points, weights, *parts, *extra)


def per_device(samples, sample_logw, references, reference_logw, dual_start, kept_tiles, tile_counts):
    n_row, n_col = lax.axis_size("row"), lax.axis_size("col")
    dim = samples.shape[1]
    own_row_blocks = samples.shape[0] // TILE
    own_col_blocks = references.shape[0] // TILE
    row_blocks, col_blocks = own_row_blocks * n_col, own_col_blocks * n_row
    chunks = TILE // LANES
    parity = lax.axis_index("row") % 2
    both = own_col_blocks % 2 == 0
    assert both or own_col_blocks == 1

    shape = jax.ShapeDtypeStruct
    depth = chunks * (dim + 1)
    kept = own_col_blocks // 2 if both else own_col_blocks
    packed_shapes = [shape((own_row_blocks, depth, LANES), jnp.float32)]
    packed_shapes += [shape((kept, depth, LANES), jnp.float32)] * (2 if both else 1)
    packed = pl.pallas_call(
        pack_kernel,
        out_shape=packed_shapes,
        in_specs=[VM] * 2,
        out_specs=[VM] * len(packed_shapes),
        compiler_params=PARAMS,
        name="pack",
    )(
        jnp.concatenate([samples.T, references.T], axis=1),
        jnp.concatenate([sample_logw, reference_logw]).reshape(-1, LANES),
    )
    x_pack, y_keep = packed[0], packed[1]
    sends = [("col", d, x_pack) for d in range(n_col - 1, 0, -1)]
    bits = [1 << i for i in range((n_row // 2).bit_length() - 1)]
    plane = [("row", 2 * bit, y_keep) for bit in reversed(bits)]
    if both:
        crossed = [("row", 2 * bit + 1, packed[2]) for bit in bits]
        plane = [send for pair in zip(plane, crossed) for send in pair]
    pace = max(1, len(plane) // (len(sends) - 1))
    order = []
    while sends or plane:
        order += sends[:1] + plane[:pace]
        sends, plane = sends[1:], plane[pace:]
    if both:
        order.append(("row", 1, packed[2]))
    got = {}
    for axis, distance, value in order:
        got[axis, distance] = swap(value, axis, distance)
    for d in range(1, n_row // 2):
        low, high = d & -d, 1 << (d.bit_length() - 1)
        if low != high:
            got["row", 2 * d] = swap(got["row", 2 * (d ^ low)], "row", 2 * low)
            if both:
                got["row", 2 * d + 1] = swap(got["row", 2 * (d ^ high) + 1], "row", 2 * high)
    own_y = [y_keep] + [got["row", 2 * d] for d in range(1, n_row // 2)]
    partner_y = [got["row", 2 * d + 1] for d in range(n_row // 2)] if both else []
    own_x = [x_pack] + [got["col", d] for d in range(1, n_col)]
    partner_x = []
    for part in own_x:
        partner_x.append(swap(part, "row", 1))
    tiles_own = jnp.concatenate([kept_tiles[0, 0], tile_counts[0]])
    tiles_partner = swap(tiles_own, "row", 1)
    dual_partner = swap(dual_start, "row", 1)
    tiles, firsts = collect_tiles(tiles_own, tiles_partner, row_blocks, col_blocks)
    xp, yp, start, wx, wy, nx, ny = prepare(
        own_x, partner_x, own_y, partner_y, dual_start, dual_partner, (row_blocks, col_blocks, dim)
    )

    row_parts = []
    col_guess = row_guess = None
    for turn in range(ITERS):
        last = turn == ITERS - 1
        (part,) = half_step(xp, yp, wx if turn else start, row_parts, col_guess, tiles, firsts[1], True, False)
        col_guess = part
        col_parts = [part] + [swap(part, "row", 2 * d) for d in range(1, n_row // 2)]
        part, *kept_total = half_step(yp, xp, wy, col_parts, row_guess, tiles, firsts[0], False, last)
        row_guess = part
        if last:
            mine, other = (
                lax.dynamic_slice_in_dim(part, side * row_blocks, row_blocks, 0) for side in (parity, 1 - parity)
            )
        else:
            mine = other = part
        part = log_sum([mine, swap(other, "row", 1)])
        row_parts = [part] + [swap(part, "col", d) for d in range(1, n_col)]

    norms = lax.dynamic_slice_in_dim(nx, parity * row_blocks, row_blocks, 0)

    def finish(norms_ref, *refs):
        *parts, out = refs
        duals = norms_ref[...] - (epsilon * ln2) * log_sum([part[...] for part in parts])
        for b in range(row_blocks):
            out[0:1, b * TILE : (b + 1) * TILE] = duals[b : b + 1, :]

    row_duals = pl.pallas_call(
        finish,
        out_shape=shape(dual_start.shape, jnp.float32),
        in_specs=[VM] * (1 + n_col),
        out_specs=VM,
        compiler_params=PARAMS,
        name="finish",
    )(norms, *row_parts)
    col_half = ny - (epsilon * ln2) * kept_total[0]
    col_other = swap(col_half, "row", 1)
    even = jnp.where(parity == 0, col_half, col_other)
    odd = jnp.where(parity == 0, col_other, col_half)
    col_duals = jnp.stack([even, odd], axis=1)
    return (row_duals, col_duals.reshape(1, -1))


def solution(mesh):
    return jax.shard_map(
        per_device,
        mesh=mesh,
        in_specs=(
            P(("row", "col"), None),
            P(("row", "col")),
            P(("row", "col"), None),
            P(("row", "col")),
            P("row", None),
            P("row", "col", None),
            P("row", "col"),
        ),
        out_specs=(P("row", None), P("col", None)),
        check_vma=False,
    )
```
